128 devices in a mesh: member: 8 (over x, core), region: 16 (over z, y).
Axes of the slice: x: 4, y: 4, z: 4, core: 2. Of those that a mesh axis runs over, the one named last changes fastest.
Arguments:
- ensemble: float32 [24, 32, 128, 512], P('member', 'region'), may hold values from -6 to 6
- obs_value: float32 [32, 128, 128], P(None, ('member', 'region')), may hold values from -6 to 6
- obs_error: float32 [32, 128, 128], P(None, ('member', 'region')), may hold values from 0.5 to 4
- obs_index: int32 [32, 128, 128], P(None, ('member', 'region')), may hold values from 0 to 511
- obs_count: int32 [32, 128], P(None, ('member', 'region')), may hold values from 1 to 128
Outputs:
- analysis: float32 [24, 32, 128, 512], P('member', 'region')
The draws below stay inside these ranges and needn't reach their ends.
Inputs may be any that keep to these rules, and one draw needn't show every extreme that they name: `obs_index`: value v names field v // (256) (0 SST, 1 SSH) at cell v mod (256) of the block, cells row-major. `obs_count`: slots below a block's count are observations; the others are padding and carry no weight.
All inputs are finite; a program needn't handle non-finite values.
Results may differ from the reference program's by a relative error of at most 0.0001.
Values sent between devices are 32-bit elements; how exact they have to be, the bound alone decides.
A program may use at most 64 MiB of HBM per device.

```python
import math
import jax
import jax.numpy as jnp
from jax import lax

SIDE = 16
OBS = 128
NS_ITERS = 6
VALS = 512
MEMBERS = 24
BROWS = 32
BCOLS = 128


def set_ends(values, own_key, low, high):
    shape = values.shape
    place = [jax.random.randint(jax.random.fold_in(own_key, axis), (), 0, shape[axis]) for axis in range(len(shape))]
    values = values.at[tuple(place)].set(low)
    longest = shape.index(max(shape))
    place[longest] = (place[longest] + 1) % shape[longest]
    return values.at[tuple(place)].set(high)


def steps_of(key, extent, cuts, smallest, top_value):
    def one(dim, shards_of):
        draws = jax.random.uniform(jax.random.fold_in(jax.random.fold_in(key, 6), dim), (shards_of,), jnp.float32, smallest / len(cuts), top_value / len(cuts))
        return jnp.repeat(jnp.exp(draws), extent[dim] // shards_of).reshape((-1,) + (1,) * (len(extent) - dim - 1))

    loudness = one(*cuts[0])
    for cut in cuts[1:]:
        loudness = loudness * one(*cut)
    return loudness


def normal_values(key, shape, width, bound, shards=(), kind=jnp.bfloat16):
    result = jax.random.normal(key, shape, jnp.float32) * width
    if len(shards) > 0:
        result = steps_of(key, shape, shards, -0.22, 0.18) * result
    return jnp.clip(result, min=-bound, max=bound).astype(kind)


def setup_inputs(seed: int = 0) -> dict:
    streams_of = jax.random.split(jax.random.key(seed), 6)
    ensemble = normal_values(streams_of[0], (MEMBERS, BROWS, BCOLS, VALS), 1.0, 6.0, ((0, 8), (1, 16)), jnp.float32)
    obs_value = normal_values(streams_of[1], (BROWS, BCOLS, OBS), 1.0, 6.0, ((1, 128),), jnp.float32)
    obs_error = jnp.clip(jnp.exp(math.log(4.0) - 2.0794415 * jax.random.uniform(streams_of[2], (BROWS, BCOLS, OBS), jnp.float32) ** steps_of(streams_of[2], (BROWS, BCOLS, OBS), ((1, 128),), -0.2, 0.2)), 0.5, 4.0)
    obs_index = set_ends(jax.random.randint(streams_of[3], (BROWS, BCOLS, OBS), 0, VALS), jax.random.fold_in(streams_of[3], 1), 0, VALS - 1).astype(jnp.int32)
    obs_count = set_ends(jax.random.randint(streams_of[4], (BROWS, BCOLS), 1, OBS + 1), jax.random.fold_in(streams_of[4], 1), 1, OBS).astype(jnp.int32)
    return dict(ensemble=ensemble, obs_value=obs_value, obs_error=obs_error, obs_index=obs_index, obs_count=obs_count)


LOC_SCALE = 12.0
INFLATION_FACTOR = 1.1

def batch_product(left, right):
    return jnp.einsum('...ij,...jk->...ik', left, right, precision=lax.Precision.HIGHEST)

def observe(ensemble, obs_value, obs_error, obs_index, obs_count):
    ens_mean = lax.optimization_barrier(jnp.mean(ensemble, axis=0))
    anomaly = ensemble - ens_mean
    slot_index = lax.broadcasted_iota(jnp.int32, obs_index.shape, 2)
    live_slot = jnp.where(slot_index < obs_count[:, :, None], 1.0, 0.0).astype(jnp.float32)
    root_weight = jnp.sqrt(live_slot / obs_error)
    full_index = jnp.broadcast_to(obs_index[None], (anomaly.shape[0],) + obs_index.shape).astype(jnp.int32)
    seen_anom = jnp.take_along_axis(anomaly, full_index, axis=3)
    seen_mean = jnp.take_along_axis(ens_mean, obs_index.astype(jnp.int32), axis=2)
    rescaled_values = root_weight[:, :, None] * jnp.moveaxis(seen_anom, 0, 2)
    innovation = root_weight * (obs_value - seen_mean)
    cell_index = obs_index % (SIDE * SIDE)
    rowpos = (cell_index // SIDE).astype(jnp.float32)
    column_position = (cell_index % SIDE).astype(jnp.float32)
    stacked = jnp.concatenate([rescaled_values, innovation[:, :, None], rowpos[:, :, None], column_position[:, :, None]], axis=2)
    return (anomaly, ens_mean, stacked)

def analyze(anomaly, ens_mean, padded):
    ensemble_members = anomaly.shape[0]
    row_count = anomaly.shape[1]
    col_count = anomaly.shape[2]
    pieces = []
    for row_step in range(3):
        for col_step in range(3):
            pieces.append(padded[row_step:row_step + row_count, col_step:col_step + col_count])
    nearby = jnp.stack(pieces, axis=2)
    rescaled_values = nearby[:, :, :, :ensemble_members]
    innovation = nearby[:, :, :, ensemble_members]
    rowpos = nearby[:, :, :, ensemble_members + 1]
    column_position = nearby[:, :, :, ensemble_members + 2]
    offset_index = jnp.arange(9, dtype=jnp.int32)
    offset_row = (offset_index // 3 - 1).astype(jnp.float32) * SIDE
    offset_col = (offset_index % 3 - 1).astype(jnp.float32) * SIDE
    half_side = SIDE // 2
    point_index = jnp.arange(4, dtype=jnp.int32)
    center_row = (point_index // 2).astype(jnp.float32) * half_side + (half_side - 1) * 0.5
    center_col = (point_index % 2).astype(jnp.float32) * half_side + (half_side - 1) * 0.5
    row_gap = offset_row[:, None] + rowpos
    col_gap = offset_col[:, None] + column_position
    distance = (row_gap[:, :, None] - center_row[:, None, None]) ** 2 + (col_gap[:, :, None] - center_col[:, None, None]) ** 2
    locality = jnp.exp(-distance / (2.0 * LOC_SCALE * LOC_SCALE))
    weighted = locality[:, :, :, :, None, :] * rescaled_values[:, :, None]
    gramian_total = jnp.einsum('rcpnko,rcnjo->rcpkj', weighted, rescaled_values, precision=lax.Precision.HIGHEST)
    drive_vec = jnp.einsum('rcpnko,rcno->rcpk', weighted, innovation, precision=lax.Precision.HIGHEST)
    identity_matrix = jnp.eye(ensemble_members, dtype=jnp.float32)
    precision_matrix = gramian_total + (ensemble_members - 1) / INFLATION_FACTOR * identity_matrix
    norm_scale = jnp.sqrt(lax.optimization_barrier(jnp.sum(precision_matrix * precision_matrix, axis=(3, 4), keepdims=True)))
    root_iter = precision_matrix / norm_scale
    inv_iter = jnp.broadcast_to(identity_matrix, precision_matrix.shape)
    for sweep_index in range(NS_ITERS):
        ns_step = 1.5 * identity_matrix - 0.5 * batch_product(inv_iter, root_iter)
        root_iter = batch_product(root_iter, ns_step)
        inv_iter = batch_product(ns_step, inv_iter)
    inv_root = inv_iter / jnp.sqrt(norm_scale)
    half_way = jnp.einsum('rcpkj,rcpj->rcpk', inv_root, drive_vec, precision=lax.Precision.HIGHEST)
    mean_w = jnp.einsum('rcpkj,rcpj->rcpk', inv_root, half_way, precision=lax.Precision.HIGHEST)
    weights = mean_w[..., :, None] + math.sqrt(ensemble_members - 1) * inv_root
    point_weights = weights.reshape(row_count, col_count, 2, 2, ensemble_members, ensemble_members)
    shaped = anomaly.reshape(ensemble_members, row_count, col_count, 2, 2, half_side, 2, half_side)
    updated = jnp.einsum('jrcvaybx,rcabjk->krcvaybx', shaped, point_weights, precision=lax.Precision.HIGHEST)
    return ens_mean[None] + updated.reshape(anomaly.shape)

def reference(ensemble, obs_value, obs_error, obs_index, obs_count):
    anomaly, ens_mean, stacked = observe(ensemble, obs_value, obs_error, obs_index, obs_count)
    padded = jnp.pad(stacked, ((1, 1), (1, 1), (0, 0), (0, 0)))

    def one_row(row_index):
        part_anom = lax.dynamic_slice_in_dim(anomaly, row_index, 1, 1)
        part_mean = lax.dynamic_slice_in_dim(ens_mean, row_index, 1, 0)
        part_pad = lax.dynamic_slice_in_dim(padded, row_index, 3, 0)
        return analyze(part_anom, part_mean, part_pad)
    row_results = lax.map(one_row, jnp.arange(BROWS, dtype=jnp.int32))
    return jnp.moveaxis(row_results[:, :, 0], 0, 1)
```

```python
import functools
import math

import jax
import jax.numpy as jnp
from jax import lax
from jax.experimental import pallas as pl
from jax.experimental.pallas import tpu as pltpu
from jax.sharding import PartitionSpec as P

MESH = pl.DeviceIdType.MESH
F32 = jnp.float32
BF16 = jnp.bfloat16

SIDE = 16
OBS = 128
NS_ITERS = 6
VALS = 512
K = 24
BROWS = 32
BCOLS = 128
LOC_SCALE = 12.0
INFLATION_FACTOR = 1.1
NM = 8
NR = 16
MINE = K // NM
ROWS = BROWS // NR
COLS = BCOLS // NM
GROUP = 8
CHUNKS = [(g, i) for g in range(COLS // GROUP) for i in range(ROWS)]
STACK = 32
PAIRS = 52 * 8


def pair_row(k, group):
    first = k // 8
    return (0, 192, 320)[first] + (k % 8) * 8 * (3 - first) + 8 * (group - first)


DRIVE = 384


def dev(m, r):
    return (lax.rem(m + NM, NM), lax.rem(r + NR, NR))


def remote(src, dst, send, recv, device):
    return pltpu.make_async_remote_copy(
        src_ref=src, dst_ref=dst, send_sem=send, recv_sem=recv, device_id=device, device_id_type=MESH
    )


def tri_product(dst, a, b, post):
    for ga in range(3):
        groups = list(range(ga, 3))

        def rows4(t, carry, ga=ga, groups=groups):
            base = (ga * 8 + t * 4) * K
            acc = [[None] * len(groups) for _ in range(4)]
            for k in range(K):
                bv = [b[pl.ds(k * K + 8 * gj, 8), :] for gj in groups]
                for u in range(4):
                    av = jnp.broadcast_to(a[pl.ds(base + u * K + k, 1), :], (8, 128))
                    for n in range(len(groups)):
                        term = av * bv[n]
                        acc[u][n] = term if acc[u][n] is None else acc[u][n] + term
            for u in range(4):
                for n, gj in enumerate(groups):
                    dst[pl.ds(base + u * K + 8 * gj, 8), :] = post(acc[u][n], ga * 8 + t * 4 + u, gj)
            return carry

        lax.fori_loop(0, 2, rows4, 0)
    fill_lower(dst)


def fill_lower(dst):
    for i in range(8, K):
        for gj in range(i // 8):
            dst[pl.ds(i * K + 8 * gj, 8), :] = dst[pl.ds(8 * gj * K + i, 8, stride=K), :]


def unit(i, gj):
    return jnp.where(lax.broadcasted_iota(jnp.int32, (8, 128), 0) + 8 * gj == i, 1.0, 0.0).astype(F32)


def newton_schulz(gram, wts, y, z, mm, tmp):
    for k in range(K):
        for gj in range(k // 8, 3):
            y[pl.ds(k * K + 8 * gj, 8), :] = gram[pl.ds(pair_row(k, gj), 8), :] + (K - 1) / INFLATION_FACTOR * unit(k, gj)
    fill_lower(y)
    square = jnp.zeros((8, 128), F32)
    for t in range(K * 3):
        v = y[pl.ds(8 * t, 8), :]
        square = square + v * v
    norm = jnp.sqrt(jnp.sum(square, axis=0, keepdims=True))
    inv_norm = 1.0 / norm
    for k in range(K):
        for gj in range(3):
            rows = pl.ds(k * K + 8 * gj, 8)
            v = y[rows, :] * inv_norm
            y[rows, :] = v
            m = 1.5 * unit(k, gj) - 0.5 * v
            mm[rows, :] = m
            z[rows, :] = m
    same = lambda v, i, gj: v
    step_of = lambda v, i, gj: 1.5 * unit(i, gj) - 0.5 * v
    tri_product(tmp, y, mm, same)

    def copy(dst, src):
        for t in range(K * 3):
            dst[pl.ds(8 * t, 8), :] = src[pl.ds(8 * t, 8), :]

    copy(y, tmp)

    def sweep(_, carry):
        tri_product(mm, z, y, step_of)
        tri_product(tmp, y, mm, same)
        copy(y, tmp)
        tri_product(tmp, mm, z, same)
        copy(z, tmp)
        return carry

    lax.fori_loop(0, NS_ITERS - 2, sweep, 0)
    tri_product(mm, z, y, step_of)
    tri_product(tmp, mm, z, same)
    scale = 1.0 / jnp.sqrt(norm)

    def apply(vector):
        acc = [jnp.zeros((8, 128), F32) for _ in range(3)]
        for k in range(K):
            row = vector[k // 8][k % 8 : k % 8 + 1, :]
            for gj in range(3):
                acc[gj] = acc[gj] + tmp[pl.ds(k * K + 8 * gj, 8), :] * row
        return [v * scale for v in acc]

    drive = [gram[pl.ds(DRIVE + 8 * gj, 8), :] for gj in range(3)]
    mean_w = apply(apply(drive))
    root = scale * math.sqrt(K - 1)
    for j in range(K):
        row = mean_w[j // 8][j % 8 : j % 8 + 1, :]
        for gj in range(3):
            rows = pl.ds(j * K + 8 * gj, 8)
            wts[rows, :] = tmp[rows, :] * root + row


def gather_chunk(x, obs, stack, means, g, i):
    cols = pl.ds(g * GROUP, GROUP)
    total = x[0, i, cols, :]
    for k in range(1, K):
        total = total + x[k, i, cols, :]
    mean = total * (1.0 / K)
    means[i, cols, :] = mean
    root_weight = obs[cols, i * 4 + 0, :]
    value = obs[cols, i * 4 + 1, :]
    index = obs[cols, i * 4 + 2, :].astype(jnp.int32)
    lane = jnp.bitwise_and(index, 127)
    tile = jnp.right_shift(index, 7)

    def pick(v):
        parts = [
            jnp.take_along_axis(v[:, 128 * t : 128 * (t + 1)], lane, axis=1, mode="promise_in_bounds") for t in range(4)
        ]
        return jnp.where(tile < 2, jnp.where(tile < 1, parts[0], parts[1]), jnp.where(tile < 3, parts[2], parts[3]))

    here = pl.ds(1 + g * GROUP, GROUP)
    for k in range(K):
        anomaly = x[k, i, cols, :] - mean
        x[k, i, cols, :] = anomaly
        stack[1 + i, here, k, :] = root_weight * pick(anomaly)
    stack[1 + i, here, K, :] = root_weight * (value - pick(mean))
    stack[1 + i, here, K + 1, :] = jnp.bitwise_and(index, SIDE * SIDE - 1).astype(F32)


def gram_column(stack, lhs, loc, gram, c, m, r):
    sub = lax.broadcasted_iota(jnp.int32, (8, 128), 0)
    point_row = jnp.right_shift(sub, 2)
    center_row = (jnp.bitwise_and(jnp.right_shift(sub, 1), 1) * 8).astype(F32) + 3.5
    center_col = (jnp.bitwise_and(sub, 1) * 8).astype(F32) + 3.5
    column = m * COLS + c - 1
    column_in = jnp.logical_and(column >= 0, column < BCOLS)
    for tr in range(ROWS + 2):
        cell = jnp.broadcast_to(stack[tr, c, pl.ds(K + 1, 1), :], (8, 128)).astype(jnp.int32)
        cell_row = jnp.right_shift(cell, 4).astype(F32)
        cell_col = jnp.bitwise_and(cell, 15).astype(F32)
        row = r * ROWS + tr - 1
        inside = jnp.logical_and(column_in, jnp.logical_and(row >= 0, row < BROWS))
        di = tr - 1 - point_row
        dy = (SIDE * di).astype(F32) + cell_row - center_row
        keep = jnp.logical_and(jnp.abs(di) <= 1, inside)
        lanes = pl.ds(tr * 128, 128)
        loc[pl.ds(pl.multiple_of(8 * c, 8), 8), lanes] = jnp.zeros((8, 128), F32)
        for e in (-1, 0, 1):
            dx = -SIDE * e + cell_col - center_col
            weight = jnp.exp((dy * dy + dx * dx) * (-1.0 / (2.0 * LOC_SCALE * LOC_SCALE)))
            loc[pl.ds(pl.multiple_of(8 * c + 16 + 8 * e, 8), 8), lanes] = jnp.where(keep, weight, 0.0)
        members = [stack[tr, c, pl.ds(8 * gj, 8), :] for gj in range(3)]
        pieces = []
        for k in range(K + 1):
            left = jnp.broadcast_to(stack[tr, c, pl.ds(k, 1), :], (8, 128))
            for gj in range(k // 8 if k < K else 0, 3):
                pieces.append(left * members[gj])
        pieces.append(jnp.zeros((8, 128), F32))
        for t in range(PAIRS // 16):
            both = jnp.concatenate(pieces[2 * t : 2 * t + 2], axis=0)
            high = both.astype(BF16)
            lhs[pl.ds(16 * t, 16), lanes] = high
            lhs[pl.ds(PAIRS + 16 * t, 16), lanes] = (both - high.astype(F32)).astype(BF16)
    weights = loc[pl.ds(24, 128), :]
    high = weights.astype(BF16)
    low = (weights - high.astype(F32)).astype(BF16)
    rhs = jnp.concatenate([high, low], axis=0)
    for half in range(2):
        rows = pl.ds(half * (PAIRS // 2), PAIRS // 2)
        dims = (((1,), (1,)), ((), ()))
        first = lax.dot_general(lhs[rows, :], rhs, dims, preferred_element_type=F32)
        second = lax.dot_general(
            lhs[pl.ds(PAIRS + half * (PAIRS // 2), PAIRS // 2), :], rhs, dims, preferred_element_type=F32
        )
        gram[rows, :] = gram[rows, :] + ((second[:, 128:] + second[:, :128]) + first[:, 128:] + first[:, :128])


def update_chunk(x, means, wts, result, g, i):
    cols = pl.ds(g * GROUP, GROUP)
    sub = lax.broadcasted_iota(jnp.int32, (8, 128), 0)
    lane = lax.broadcasted_iota(jnp.int32, (8, 128), 1)
    base = (g * GROUP + sub) * 8 + i * 4 + jnp.bitwise_and(jnp.right_shift(lane, 3), 1)
    for h in range(2):
        index = base + 2 * h

        def some(t, carry, h=h, index=index):
            acc = [[means[i, cols, pl.ds(128 * (2 * f + h), 128)] for f in range(2)] for _ in range(6)]
            for j in range(K):
                xs = [x[j, i, cols, pl.ds(128 * (2 * f + h), 128)] for f in range(2)]
                for u in range(6):
                    row = jnp.broadcast_to(wts[pl.ds(j * K + t * 6 + u, 1), :], (8, 128))
                    wv = jnp.take_along_axis(row, index, axis=1, mode="promise_in_bounds")
                    for f in range(2):
                        acc[u][f] = acc[u][f] + wv * xs[f]
            for u in range(6):
                for f in range(2):
                    result[t * 6 + u, i, cols, pl.ds(128 * (2 * f + h), 128)] = acc[u][f]
            return carry

        lax.fori_loop(0, K // 6, some, 0)


def kernel(
    ens, packed, out,
    x, obs, stack, means, lhs, loc, gram, wts, y, z, mm, tmp, result,
    obs_send, obs_recv, in_send, in_recv, own_in, halo_send, halo_recv, out_send, out_recv, own_out,
):
    m = lax.axis_index("member")
    r = lax.axis_index("region")

    barrier = pltpu.get_barrier_semaphore()
    around = [dev(m + d, r) for d in range(1, NM)] + [dev(m, r + d) for d in range(1, NR)]
    around += [dev(m + a, r + b) for a in (-1, 1) for b in (-1, 1)]
    for device in around:
        pl.semaphore_signal(barrier, inc=1, device_id=device, device_id_type=MESH)
    pl.semaphore_wait(barrier, len(around))

    def obs_copy(d):
        other = lax.rem(r + d, NR)
        return remote(packed.at[other], obs.at[r], obs_send.at[d], obs_recv.at[d], (m, other))

    for d in range(1, NR):
        obs_copy(d).start()

    def in_copy(q, d):
        g, i = CHUNKS[q]
        other = lax.rem(m + d, NM)
        src = ens.at[:, i, pl.ds(pl.multiple_of(other * COLS + g * GROUP, GROUP), GROUP), :]
        dst = x.at[pl.ds(m * MINE, MINE), i, pl.ds(g * GROUP, GROUP), :]
        return remote(src, dst, in_send.at[q, d], in_recv.at[q, d], (other, r))

    def own_copy(q):
        g, i = CHUNKS[q]
        src = ens.at[:, i, pl.ds(pl.multiple_of(m * COLS + g * GROUP, GROUP), GROUP), :]
        dst = x.at[pl.ds(m * MINE, MINE), i, pl.ds(g * GROUP, GROUP), :]
        return pltpu.make_async_copy(src, dst, own_in.at[q])

    for q in range(len(CHUNKS)):
        for d in range(1, NM):
            in_copy(q, d).start()
        own_copy(q).start()

    obs[r] = packed[r]
    loc[...] = jnp.zeros_like(loc)
    gram[...] = jnp.zeros_like(gram)
    for d in range(1, NR):
        obs_copy(d).wait_recv()

    def row_halo(g, i):
        where = pl.ds(1 + g * GROUP, GROUP)
        to = 3 if i == 0 else 0
        n = 2 * g + i
        return remote(
            stack.at[1 + i, where], stack.at[to, where], halo_send.at[n], halo_recv.at[n], dev(m, r + (-1 if i == 0 else 1))
        )

    def side_halo(g, n):
        col, to, a = (1, COLS + 1, -1) if g == 0 else (COLS, 0, 1)
        if n == 0:
            src, dst, b = stack.at[pl.ds(1, 2), col], stack.at[pl.ds(1, 2), to], 0
        elif n == 1:
            src, dst, b = stack.at[1, col], stack.at[3, to], -1
        else:
            src, dst, b = stack.at[2, col], stack.at[0, to], 1
        s = 4 + 3 * g + n
        return remote(src, dst, halo_send.at[s], halo_recv.at[s], dev(m + a, r + b))

    halos = []
    for q, (g, i) in enumerate(CHUNKS):
        own_copy(q).wait()
        for d in range(1, NM):
            in_copy(q, d).wait_recv()
        gather_chunk(x, obs, stack, means, g, i)
        new = [row_halo(g, i)]
        if i == ROWS - 1:
            new += [side_halo(g, n) for n in range(3)]
        for copy in new:
            copy.start()
        halos += new
    for copy in halos:
        copy.wait_recv()

    def column(c, carry):
        gram_column(stack, lhs, loc, gram, c, m, r)
        return carry

    lax.fori_loop(0, COLS + 2, column, 0)
    newton_schulz(gram, wts, y, z, mm, tmp)

    def out_copy(q, d):
        g, i = CHUNKS[q]
        other = lax.rem(m + d, NM)
        src = result.at[pl.ds(other * MINE, MINE), i, pl.ds(g * GROUP, GROUP), :]
        dst = out.at[:, i, pl.ds(pl.multiple_of(m * COLS + g * GROUP, GROUP), GROUP), :]
        return remote(src, dst, out_send.at[q, d], out_recv.at[q, d], (other, r))

    def keep_copy(q):
        g, i = CHUNKS[q]
        src = result.at[pl.ds(m * MINE, MINE), i, pl.ds(g * GROUP, GROUP), :]
        dst = out.at[:, i, pl.ds(pl.multiple_of(m * COLS + g * GROUP, GROUP), GROUP), :]
        return pltpu.make_async_copy(src, dst, own_out.at[q])

    for q, (g, i) in enumerate(CHUNKS):
        update_chunk(x, means, wts, result, g, i)
        for d in range(1, NM):
            out_copy(q, d).start()
        keep_copy(q).start()

    for d in range(1, NR):
        obs_copy(d).wait_send()
    for copy in halos:
        copy.wait_send()
    for q in range(len(CHUNKS)):
        for d in range(1, NM):
            in_copy(q, d).wait_send()
            out_copy(q, d).wait_send()
            out_copy(q, d).wait_recv()
        keep_copy(q).wait()


def local(ensemble, obs_value, obs_error, obs_index, obs_count):
    slot = lax.broadcasted_iota(jnp.int32, obs_index.shape, 2)
    live = jnp.where(slot < obs_count[:, :, None], 1.0, 0.0).astype(F32)
    root_weight = jnp.sqrt(live / obs_error)
    packed = jnp.concatenate([root_weight, obs_value, obs_index.astype(F32), jnp.zeros_like(obs_value)], axis=1)
    packed = packed.reshape(NR, 4 * ROWS, OBS)
    dma = pltpu.SemaphoreType.DMA
    n = len(CHUNKS)
    square = pltpu.VMEM((K * K, 128), F32)
    return pl.pallas_call(
        kernel,
        out_shape=jax.ShapeDtypeStruct(ensemble.shape, F32),
        in_specs=[pl.BlockSpec(memory_space=pl.ANY), pl.BlockSpec(memory_space=pltpu.VMEM)],
        out_specs=pl.BlockSpec(memory_space=pl.ANY),
        scratch_shapes=[
            pltpu.VMEM((K, ROWS, COLS, VALS), F32),
            pltpu.VMEM((COLS, 4 * ROWS, OBS), F32),
            pltpu.VMEM((ROWS + 2, COLS + 2, STACK, OBS), F32),
            pltpu.VMEM((ROWS, COLS, VALS), F32),
            pltpu.VMEM((2 * PAIRS, 512), BF16),
            pltpu.VMEM((168, 512), F32),
            pltpu.VMEM((PAIRS, 128), F32),
            square, square, square, square, square,
            pltpu.VMEM((K, ROWS, COLS, VALS), F32),
            dma((NR,)), dma((NR,)), dma((n, NM)), dma((n, NM)), dma((n,)),
            dma((10,)), dma((10,)), dma((n, NM)), dma((n, NM)), dma((n,)),
        ],
        compiler_params=pltpu.CompilerParams(collective_id=0, has_side_effects=True),
    )(ensemble, packed)


def solution(mesh):
    return jax.shard_map(
        local,
        mesh=mesh,
        in_specs=(
            P("member", "region", None, None),
            P(None, ("member", "region"), None),
            P(None, ("member", "region"), None),
            P(None, ("member", "region"), None),
            P(None, ("member", "region")),
        ),
        out_specs=P("member", "region", None, None),
        check_vma=False,
    )
```

```python
import functools
import math

import jax
import jax.numpy as jnp
from jax import lax
from jax.experimental import pallas as pl
from jax.experimental.pallas import tpu as pltpu
from jax.sharding import PartitionSpec as P

MESH = pl.DeviceIdType.MESH
F32 = jnp.float32
BF16 = jnp.bfloat16

SIDE = 16
OBS = 128
NS_ITERS = 6
VALS = 512
K = 24
BROWS = 32
BCOLS = 128
LOC_SCALE = 12.0
INFLATION_FACTOR = 1.1
NM = 8
NR = 16
MINE = K // NM
ROWS = BROWS // NR
COLS = BCOLS // NM
GROUP = 8
CHUNKS = [(g, i) for g in range(COLS // GROUP) for i in range(ROWS)]
STACK = 32
PAIRS = 52 * 8


def pair_row(k, group):
    first = k // 8
    return (0, 192, 320)[first] + (k % 8) * 8 * (3 - first) + 8 * (group - first)


DRIVE = 384


def dev(m, r):
    return (lax.rem(m + NM, NM), lax.rem(r + NR, NR))


def remote(src, dst, send, recv, device):
    return pltpu.make_async_remote_copy(
        src_ref=src, dst_ref=dst, send_sem=send, recv_sem=recv, device_id=device, device_id_type=MESH
    )


def tri_product(dst, a, b, post):
    for ga, height in ((0, 4), (1, 4), (2, 8)):
        groups = list(range(ga, 3))
        for first in range(8 * ga, 8 * ga + 8, height):
            acc = [[None] * len(groups) for _ in range(height)]
            for k in range(K):
                bv = [b[pl.ds(k * K + 8 * gj, 8), :] for gj in groups]
                for u in range(height):
                    av = jnp.broadcast_to(a[pl.ds((first + u) * K + k, 1), :], (8, 128))
                    for n in range(len(groups)):
                        term = av * bv[n]
                        acc[u][n] = term if acc[u][n] is None else acc[u][n] + term
            for u in range(height):
                for n, gj in enumerate(groups):
                    dst[pl.ds((first + u) * K + 8 * gj, 8), :] = post(acc[u][n], first + u, gj)
    fill_lower(dst)


def fill_lower(dst):
    for i in range(8, K):
        for gj in range(i // 8):
            dst[pl.ds(i * K + 8 * gj, 8), :] = dst[pl.ds(8 * gj * K + i, 8, stride=K), :]


def unit(i, gj):
    if i // 8 != gj:
        return jnp.zeros((8, 128), F32)
    return jnp.where(lax.broadcasted_iota(jnp.int32, (8, 128), 0) == i % 8, 1.0, 0.0).astype(F32)


def same(v, i, gj):
    return v


def newton_schulz(gram, wts, p, s, t, z, rest):
    square = jnp.zeros((8, 128), F32)
    for k in range(K):
        for gj in range(k // 8, 3):
            v = gram[pl.ds(pair_row(k, gj), 8), :] + (K - 1) / INFLATION_FACTOR * unit(k, gj)
            p[pl.ds(k * K + 8 * gj, 8), :] = v
            square = square + v * v * (1.0 if gj == k // 8 else 2.0)
    norm = jnp.sqrt(jnp.sum(square, axis=0, keepdims=True))
    inv_norm = 1.0 / norm
    for k in range(K):
        for gj in range(k // 8, 3):
            rows = pl.ds(k * K + 8 * gj, 8)
            p[rows, :] = p[rows, :] * inv_norm
    fill_lower(p)

    def square_of(v, i, gj):
        rows = pl.ds(i * K + 8 * gj, 8)
        rest[rows, :] = 1.6875 * unit(i, gj) - 0.5625 * p[rows, :] + 0.0625 * v
        return v

    def factor_of(v, i, gj):
        return v + (2.25 * unit(i, gj) - 2.4375 * p[pl.ds(i * K + 8 * gj, 8), :])

    def factor(dst):
        tri_product(s, p, p, square_of)
        fill_lower(rest)
        tri_product(dst, s, rest, factor_of)

    factor(z)
    tri_product(t, p, z, same)
    tri_product(p, t, z, same)
    factor(t)
    tri_product(s, p, t, same)
    tri_product(p, s, t, same)
    tri_product(wts, z, t, same)
    factor(t)
    tri_product(z, wts, t, same)
    scale = 1.0 / jnp.sqrt(norm)

    def apply(vector):
        acc = [jnp.zeros((8, 128), F32) for _ in range(3)]
        for k in range(K):
            row = vector[k // 8][k % 8 : k % 8 + 1, :]
            for gj in range(3):
                acc[gj] = acc[gj] + z[pl.ds(k * K + 8 * gj, 8), :] * row
        return [v * scale for v in acc]

    drive = [gram[pl.ds(DRIVE + 8 * gj, 8), :] for gj in range(3)]
    mean_w = apply(apply(drive))
    root = scale * math.sqrt(K - 1)
    for j in range(K):
        row = mean_w[j // 8][j % 8 : j % 8 + 1, :]
        for gj in range(3):
            rows = pl.ds(j * K + 8 * gj, 8)
            wts[rows, :] = z[rows, :] * root + row


def gather_chunk(x, obs, stack, means, g, i):
    cols = pl.ds(g * GROUP, GROUP)
    total = x[0, i, cols, :]
    for k in range(1, K):
        total = total + x[k, i, cols, :]
    mean = total * (1.0 / K)
    means[i, cols, :] = mean
    root_weight = obs[cols, i * 4 + 0, :]
    value = obs[cols, i * 4 + 1, :]
    index = obs[cols, i * 4 + 2, :].astype(jnp.int32)
    lane = jnp.bitwise_and(index, 127)
    tile = jnp.right_shift(index, 7)

    def pick(v):
        parts = [
            jnp.take_along_axis(v[:, 128 * t : 128 * (t + 1)], lane, axis=1, mode="promise_in_bounds") for t in range(4)
        ]
        return jnp.where(tile < 2, jnp.where(tile < 1, parts[0], parts[1]), jnp.where(tile < 3, parts[2], parts[3]))

    here = pl.ds(1 + g * GROUP, GROUP)
    for k in range(K):
        anomaly = x[k, i, cols, :] - mean
        x[k, i, cols, :] = anomaly
        stack[1 + i, here, k, :] = root_weight * pick(anomaly)
    stack[1 + i, here, K, :] = root_weight * (value - pick(mean))
    stack[1 + i, here, K + 1, :] = jnp.bitwise_and(index, SIDE * SIDE - 1).astype(F32)


def gram_blocks(stack, lhs, loc, gram, blocks, m, r):
    sub = lax.broadcasted_iota(jnp.int32, (8, 128), 0)
    point_row = jnp.right_shift(sub, 2)
    center_row = (jnp.bitwise_and(jnp.right_shift(sub, 1), 1) * 8).astype(F32) + 3.5
    center_col = (jnp.bitwise_and(sub, 1) * 8).astype(F32) + 3.5
    zero = jnp.zeros((8, 128), F32)
    blank = jnp.zeros((16, 128), BF16)
    for n, (tr, c) in enumerate(blocks):
        lanes = pl.ds(n * 128, 128)
        cell = jnp.broadcast_to(stack[tr, c, pl.ds(K + 1, 1), :], (8, 128)).astype(jnp.int32)
        cell_row = jnp.right_shift(cell, 4).astype(F32)
        cell_col = jnp.bitwise_and(cell, 15).astype(F32)
        row = r * ROWS + tr - 1
        column = m * COLS + c - 1
        inside = jnp.logical_and(jnp.logical_and(column >= 0, column < BCOLS), jnp.logical_and(row >= 0, row < BROWS))
        di = tr - 1 - point_row
        dy = (SIDE * di).astype(F32) + cell_row - center_row
        keep = jnp.logical_and(jnp.abs(di) <= 1, inside)
        reach = {}
        for e in (-1, 0, 1):
            if 0 <= c - 1 + e < COLS:
                dx = cell_col - center_col - float(SIDE * e)
                weight = jnp.exp((dy * dy + dx * dx) * (-1.0 / (2.0 * LOC_SCALE * LOC_SCALE)))
                reach[c - 1 + e] = jnp.where(keep, weight, 0.0)
        for tile in range(COLS // 2):
            if 2 * tile in reach or 2 * tile + 1 in reach:
                both = jnp.concatenate([reach.get(2 * tile, zero), reach.get(2 * tile + 1, zero)], axis=0)
                high = both.astype(BF16)
                low = (both - high.astype(F32)).astype(BF16)
            else:
                high = low = blank
            loc[pl.ds(16 * tile, 16), lanes] = high
            loc[pl.ds(128 + 16 * tile, 16), lanes] = low
        members = [stack[tr, c, pl.ds(8 * gj, 8), :] for gj in range(3)]
        pieces = []
        for k in range(K + 1):
            left = jnp.broadcast_to(stack[tr, c, pl.ds(k, 1), :], (8, 128))
            for gj in range(k // 8 if k < K else 0, 3):
                pieces.append(left * members[gj])
        pieces.append(zero)
        for t in range(PAIRS // 16):
            both = jnp.concatenate(pieces[2 * t : 2 * t + 2], axis=0)
            high = both.astype(BF16)
            lhs[pl.ds(16 * t, 16), lanes] = high
            lhs[pl.ds(PAIRS + 16 * t, 16), lanes] = (both - high.astype(F32)).astype(BF16)
    depth = pl.ds(0, 128 * len(blocks))
    dims = (((1,), (1,)), ((), ()))
    total = lax.dot_general(lhs[:, depth], loc[:, depth], dims, preferred_element_type=F32)
    high, low = total[:PAIRS], total[PAIRS:]
    gram[...] = gram[...] + ((low[:, 128:] + low[:, :128]) + high[:, 128:] + high[:, :128])


def update_members(x, means, wts, result, g, i, others):
    cols = pl.ds(pl.multiple_of(g * GROUP, GROUP), GROUP)
    sub = lax.broadcasted_iota(jnp.int32, (8, 128), 0)
    lane = lax.broadcasted_iota(jnp.int32, (8, 128), 1)
    base = (g * GROUP + sub) * 8 + i * 4 + jnp.bitwise_and(jnp.right_shift(lane, 3), 1)
    members = [other * MINE + u for other in others for u in range(MINE)]
    for h in range(2):
        index = base + 2 * h
        acc = [[means[i, cols, pl.ds(128 * (2 * f + h), 128)] for f in range(2)] for _ in members]
        for j in range(K):
            xs = [x[j, i, cols, pl.ds(128 * (2 * f + h), 128)] for f in range(2)]
            for u, k in enumerate(members):
                row = jnp.broadcast_to(wts[pl.ds(j * K + k, 1), :], (8, 128))
                wv = jnp.take_along_axis(row, index, axis=1, mode="promise_in_bounds")
                for f in range(2):
                    acc[u][f] = acc[u][f] + wv * xs[f]
        for u, k in enumerate(members):
            for f in range(2):
                result[k, i, cols, pl.ds(128 * (2 * f + h), 128)] = acc[u][f]


def kernel(
    ens, value_in, error_in, index_in, count, out,
    value, error, index, load,
    x, obs, packed, stack, means, lhs, loc, gram, wts, y, z, mm, tmp, rest, result,
    obs_send, obs_recv, in_send, in_recv, own_in, halo_send, halo_recv, out_send, out_recv, own_out,
):
    m = lax.axis_index("member")
    r = lax.axis_index("region")

    loads = [
        pltpu.make_async_copy(src, dst, load.at[n])
        for n, (src, dst) in enumerate(((value_in, value), (error_in, error), (index_in, index)))
    ]
    for copy in loads:
        copy.start()
    barrier = pltpu.get_barrier_semaphore()
    around = [dev(m + d, r) for d in range(1, NM)] + [dev(m, r + d) for d in range(1, NR)]
    around += [dev(m + a, r + b) for a in (-1, 1) for b in (-1, 1)]
    for device in around:
        pl.semaphore_signal(barrier, inc=1, device_id=device, device_id_type=MESH)
    for copy in loads:
        copy.wait()
    sub = lax.broadcasted_iota(jnp.int32, (8, OBS), 0)
    slot = lax.broadcasted_iota(jnp.int32, (8, OBS), 1)
    for n in range(BROWS // 8):
        rows = pl.ds(8 * n, 8)
        limit = jnp.zeros((8, OBS), jnp.int32)
        for u in range(8):
            limit = jnp.where(sub == u, count[0, 8 * n + u], limit)
        live = jnp.where(slot < limit, 1.0, 0.0).astype(F32)
        fields = (jnp.sqrt(live / error[rows, 0, :]), value[rows, 0, :], index[rows, 0, :].astype(F32))
        for f, field in enumerate(fields):
            for u in range(8):
                to = 8 * n + u
                packed[to // ROWS, to % ROWS * 4 + f, :] = field[u]
    pl.semaphore_wait(barrier, len(around))

    def obs_copy(d):
        other = lax.rem(r + d, NR)
        return remote(packed.at[other], obs.at[r], obs_send.at[d], obs_recv.at[d], (m, other))

    for d in range(1, NR):
        obs_copy(d).start()

    def in_copy(q, d):
        g, i = CHUNKS[q]
        other = lax.rem(m + d, NM)
        src = ens.at[:, i, pl.ds(pl.multiple_of(other * COLS + g * GROUP, GROUP), GROUP), :]
        dst = x.at[pl.ds(m * MINE, MINE), i, pl.ds(g * GROUP, GROUP), :]
        return remote(src, dst, in_send.at[q, d], in_recv.at[q, d], (other, r))

    def own_copy(q):
        g, i = CHUNKS[q]
        src = ens.at[:, i, pl.ds(pl.multiple_of(m * COLS + g * GROUP, GROUP), GROUP), :]
        dst = x.at[pl.ds(m * MINE, MINE), i, pl.ds(g * GROUP, GROUP), :]
        return pltpu.make_async_copy(src, dst, own_in.at[q])

    def send_in(q):
        for d in range(1, NM):
            in_copy(q, d).start()
        own_copy(q).start()

    send_in(0)
    send_in(1)
    obs[r] = packed[r]
    gram[...] = jnp.zeros_like(gram)
    for d in range(1, NR):
        obs_copy(d).wait_recv()

    def row_halo(g, i):
        where = pl.ds(1 + g * GROUP, GROUP)
        to = 3 if i == 0 else 0
        n = 2 * g + i
        return remote(
            stack.at[1 + i, where], stack.at[to, where], halo_send.at[n], halo_recv.at[n], dev(m, r + (-1 if i == 0 else 1))
        )

    def side_halo(g, n):
        col, to, a = (1, COLS + 1, -1) if g == 0 else (COLS, 0, 1)
        if n == 0:
            src, dst, b = stack.at[pl.ds(1, 2), col], stack.at[pl.ds(1, 2), to], 0
        elif n == 1:
            src, dst, b = stack.at[1, col], stack.at[3, to], -1
        else:
            src, dst, b = stack.at[2, col], stack.at[0, to], 1
        s = 4 + 3 * g + n
        return remote(src, dst, halo_send.at[s], halo_recv.at[s], dev(m + a, r + b))

    halos = []

    def arrive(q):
        g, i = CHUNKS[q]
        own_copy(q).wait()
        for d in range(1, NM):
            in_copy(q, d).wait_recv()
        gather_chunk(x, obs, stack, means, g, i)
        new = [row_halo(g, i)]
        if i == ROWS - 1:
            new += [side_halo(g, n) for n in range(3)]
        for copy in new:
            copy.start()
        halos.extend(new)
        if q + 2 < len(CHUNKS):
            send_in(q + 2)

    def add(blocks):
        gram_blocks(stack, lhs, loc, gram, blocks, m, r)

    def own(q):
        g, i = CHUNKS[q]
        return [(1 + i, 1 + g * GROUP + c) for c in range(GROUP)]

    def beyond(q):
        g, i = CHUNKS[q]
        return [(3 if i == 0 else 0, 1 + g * GROUP + c) for c in range(GROUP)]

    arrive(0)
    arrive(1)
    row_halo(*CHUNKS[0]).wait_recv()
    add(own(0) + beyond(0))
    arrive(2)
    row_halo(*CHUNKS[1]).wait_recv()
    add(own(1) + beyond(1))
    arrive(3)
    row_halo(*CHUNKS[2]).wait_recv()
    for n in range(3):
        side_halo(0, n).wait_recv()
    add(own(2) + beyond(2) + own(3) + [(tr, COLS + 1) for tr in range(4)])
    row_halo(*CHUNKS[3]).wait_recv()
    for n in range(3):
        side_halo(1, n).wait_recv()
    add(beyond(3) + [(tr, 0) for tr in range(4)])
    newton_schulz(gram, wts, y, z, mm, tmp, rest)

    def out_copy(q, d):
        g, i = q // ROWS, q % ROWS
        other = lax.rem(m + d, NM)
        src = result.at[pl.ds(other * MINE, MINE), i, pl.ds(pl.multiple_of(g * GROUP, GROUP), GROUP), :]
        dst = out.at[:, i, pl.ds(pl.multiple_of(m * COLS + g * GROUP, GROUP), GROUP), :]
        return remote(src, dst, out_send.at[q, d], out_recv.at[q, d], (other, r))

    def keep_copy(q):
        g, i = q // ROWS, q % ROWS
        src = result.at[pl.ds(m * MINE, MINE), i, pl.ds(pl.multiple_of(g * GROUP, GROUP), GROUP), :]
        dst = out.at[:, i, pl.ds(pl.multiple_of(m * COLS + g * GROUP, GROUP), GROUP), :]
        return pltpu.make_async_copy(src, dst, own_out.at[q])

    def chunk_out(q, carry):
        for pair in ((1, 2), (3, 4), (5, 6), (7, 0)):
            update_members(x, means, wts, result, q // ROWS, q % ROWS, [lax.rem(m + d, NM) for d in pair])
            for d in pair:
                (out_copy(q, d) if d else keep_copy(q)).start()
        return carry

    lax.fori_loop(0, len(CHUNKS), chunk_out, 0)

    for d in range(1, NR):
        obs_copy(d).wait_send()
    for copy in halos:
        copy.wait_send()
    for q in range(len(CHUNKS)):
        for d in range(1, NM):
            in_copy(q, d).wait_send()
            out_copy(q, d).wait_send()
            out_copy(q, d).wait_recv()
        keep_copy(q).wait()


def local(ensemble, obs_value, obs_error, obs_index, obs_count):
    dma = pltpu.SemaphoreType.DMA
    n = len(CHUNKS)
    square = pltpu.VMEM((K * K, 128), F32)
    return pl.pallas_call(
        kernel,
        out_shape=jax.ShapeDtypeStruct(ensemble.shape, F32),
        in_specs=[pl.BlockSpec(memory_space=pltpu.MemorySpace.HBM)] * 4 + [pl.BlockSpec(memory_space=pltpu.SMEM)],
        out_specs=pl.BlockSpec(memory_space=pl.ANY),
        scratch_shapes=[
            pltpu.VMEM((BROWS, 1, OBS), F32), pltpu.VMEM((BROWS, 1, OBS), F32), pltpu.VMEM((BROWS, 1, OBS), jnp.int32), dma((3,)),
            pltpu.VMEM((K, ROWS, COLS, VALS), F32),
            pltpu.VMEM((COLS, 4 * ROWS, OBS), F32),
            pltpu.VMEM((NR, 4 * ROWS, OBS), F32),
            pltpu.VMEM((ROWS + 2, COLS + 2, STACK, OBS), F32),
            pltpu.VMEM((ROWS, COLS, VALS), F32),
            pltpu.VMEM((2 * PAIRS, 28 * 128), BF16),
            pltpu.VMEM((256, 28 * 128), BF16),
            pltpu.VMEM((PAIRS, 128), F32),
            square, square, square, square, square, square,
            pltpu.VMEM((K, ROWS, COLS, VALS), F32),
            dma((NR,)), dma((NR,)), dma((n, NM)), dma((n, NM)), dma((n,)),
            dma((10,)), dma((10,)), dma((n, NM)), dma((n, NM)), dma((n,)),
        ],
        compiler_params=pltpu.CompilerParams(collective_id=0, has_side_effects=True),
    )(ensemble, obs_value, obs_error, obs_index, obs_count.reshape(1, BROWS))


def solution(mesh):
    return jax.shard_map(
        local,
        mesh=mesh,
        in_specs=(
            P("member", "region", None, None),
            P(None, ("member", "region"), None),
            P(None, ("member", "region"), None),
            P(None, ("member", "region"), None),
            P(None, ("member", "region")),
        ),
        out_specs=P("member", "region", None, None),
        check_vma=False,
    )
```

```python
import functools
import math

import jax
import jax.numpy as jnp
from jax import lax
from jax.experimental import pallas as pl
from jax.experimental.pallas import tpu as pltpu
from jax.sharding import PartitionSpec as P

MESH = pl.DeviceIdType.MESH
F32 = jnp.float32
BF16 = jnp.bfloat16

SIDE = 16
OBS = 128
NS_ITERS = 6
VALS = 512
K = 24
BROWS = 32
BCOLS = 128
LOC_SCALE = 12.0
INFLATION_FACTOR = 1.1
NM = 8
NR = 16
MINE = K // NM
ROWS = BROWS // NR
COLS = BCOLS // NM
GROUP = 8
CHUNKS = [(g, i) for g in range(COLS // GROUP) for i in range(ROWS)]
AT = GROUP - 1
TERMS = [(a, b, d) for a in range(3) for b in range(a, 3) for d in range(8 if b > a else 5)]
DRIVE = 8 * len(TERMS)
PAIRS = DRIVE + K
DEEP = 8


def dev(m, r):
    return (lax.rem(m + NM, NM), lax.rem(r + NR, NR))


def remote(src, dst, send, recv, device):
    return pltpu.make_async_remote_copy(
        src_ref=src, dst_ref=dst, send_sem=send, recv_sem=recv, device_id=device, device_id_type=MESH
    )


def tri_product(dst, a, b, post):
    for ga, height in ((0, 4), (1, 4), (2, 8)):
        groups = list(range(ga, 3))
        for first in range(8 * ga, 8 * ga + 8, height):
            acc = [[None] * len(groups) for _ in range(height)]
            for k in range(K):
                bv = [b[pl.ds(k * K + 8 * gj, 8), :] for gj in groups]
                for u in range(height):
                    av = jnp.broadcast_to(a[pl.ds((first + u) * K + k, 1), :], (8, 128))
                    for n in range(len(groups)):
                        term = av * bv[n]
                        acc[u][n] = term if acc[u][n] is None else acc[u][n] + term
            for u in range(height):
                for n, gj in enumerate(groups):
                    dst[pl.ds((first + u) * K + 8 * gj, 8), :] = post(acc[u][n], first + u, gj)
    fill_lower(dst)


def fill_lower(dst):
    for i in range(8, K):
        for gj in range(i // 8):
            dst[pl.ds(i * K + 8 * gj, 8), :] = dst[pl.ds(8 * gj * K + i, 8, stride=K), :]


def unit(i, gj):
    if i // 8 != gj:
        return jnp.zeros((8, 128), F32)
    return jnp.where(lax.broadcasted_iota(jnp.int32, (8, 128), 0) == i % 8, 1.0, 0.0).astype(F32)


def same(v, i, gj):
    return v


def newton_schulz(gram, wts, p, s, t, z, rest):
    square = jnp.zeros((8, 128), F32)
    for ga in range(3):
        for gb in range(ga, 3):
            base = 8 * TERMS.index((ga, gb, 0))
            source, start = gram, base
            if ga == gb:
                source, start = rest, 64 * ga
                for d in range(8):
                    v = gram[pl.ds(base + 8 * min(d, 8 - d), 8), :]
                    rest[pl.ds(start + 8 * d, 8), :] = pltpu.roll(v, 8 - d, 0) if d > 4 else v
            for u in range(8):
                k = 8 * ga + u
                v = source[pl.ds(start + u, 8, stride=8), :]
                v = pltpu.roll(v, u, 0) if u else v
                if ga == gb:
                    v = v + (K - 1) / INFLATION_FACTOR * unit(k, gb)
                p[pl.ds(k * K + 8 * gb, 8), :] = v
                square = square + v * v * (1.0 if ga == gb else 2.0)
    norm = jnp.sqrt(jnp.sum(square, axis=0, keepdims=True))
    inv_norm = 1.0 / norm
    for k in range(K):
        for gj in range(k // 8, 3):
            rows = pl.ds(k * K + 8 * gj, 8)
            p[rows, :] = p[rows, :] * inv_norm
    fill_lower(p)

    def square_of(v, i, gj):
        rows = pl.ds(i * K + 8 * gj, 8)
        rest[rows, :] = 1.6875 * unit(i, gj) - 0.5625 * p[rows, :] + 0.0625 * v
        return v

    def factor_of(v, i, gj):
        return v + (2.25 * unit(i, gj) - 2.4375 * p[pl.ds(i * K + 8 * gj, 8), :])

    def factor(dst):
        tri_product(s, p, p, square_of)
        fill_lower(rest)
        tri_product(dst, s, rest, factor_of)

    factor(z)
    tri_product(t, p, z, same)
    tri_product(p, t, z, same)
    factor(t)
    tri_product(s, p, t, same)
    tri_product(p, s, t, same)
    tri_product(wts, z, t, same)
    factor(t)
    tri_product(z, wts, t, same)
    scale = 1.0 / jnp.sqrt(norm)

    def apply(vector):
        acc = [jnp.zeros((8, 128), F32) for _ in range(3)]
        for k in range(K):
            row = vector[k // 8][k % 8 : k % 8 + 1, :]
            for gj in range(3):
                acc[gj] = acc[gj] + z[pl.ds(k * K + 8 * gj, 8), :] * row
        return [v * scale for v in acc]

    drive = [gram[pl.ds(DRIVE + 8 * gj, 8), :] for gj in range(3)]
    mean_w = apply(apply(drive))
    root = scale * math.sqrt(K - 1)
    for j in range(K):
        row = mean_w[j // 8][j % 8 : j % 8 + 1, :]
        for gj in range(3):
            rows = pl.ds(j * K + 8 * gj, 8)
            wts[rows, :] = z[rows, :] * root + row


def gather_group(mine, places, seen_out, m, g):
    for other in range(NM):
        cols = pl.ds(other * COLS + g * GROUP, GROUP)
        for i in range(ROWS):
            index = places[i, cols, :].astype(jnp.int32)
            lane = jnp.bitwise_and(index, 127)
            tile = jnp.right_shift(index, 7)
            for u in range(MINE):
                v = [
                    jnp.take_along_axis(mine[u, i, cols, pl.ds(128 * t, 128)], lane, axis=1, mode="promise_in_bounds")
                    for t in range(4)
                ]
                low, high = jnp.where(tile < 1, v[0], v[1]), jnp.where(tile < 3, v[2], v[3])
                seen_out[g, other, u, i] = jnp.where(tile < 2, low, high)


def stack_group(seen, obs, stack, extra, g):
    cols = pl.ds(g * GROUP, GROUP)
    here = pl.ds(1 + g * GROUP, GROUP)
    for i in range(ROWS):
        total = seen[g, 0, i]
        for k in range(1, K):
            total = total + seen[g, k, i]
        mean = total * (1.0 / K)
        root_weight = obs[cols, i * 4 + 0, :]
        for k in range(K):
            stack[1 + i, here, k, :] = root_weight * (seen[g, k, i] - mean)
        index = obs[cols, i * 4 + 2, :].astype(jnp.int32)
        extra[1 + i, 0, pl.ds((1 + g) * GROUP, GROUP), :] = root_weight * (obs[cols, i * 4 + 1, :] - mean)
        extra[1 + i, 1, pl.ds((1 + g) * GROUP, GROUP), :] = jnp.bitwise_and(index, SIDE * SIDE - 1).astype(F32)


def center_chunk(x, means, g, i):
    cols = pl.ds(pl.multiple_of(g * GROUP, GROUP), GROUP)
    for t in range(4):
        lanes = pl.ds(128 * t, 128)
        total = x[0, i, cols, lanes]
        for k in range(1, K):
            total = total + x[k, i, cols, lanes]
        mean = total * (1.0 / K)
        means[i, cols, lanes] = mean
        for k in range(K):
            x[k, i, cols, lanes] = x[k, i, cols, lanes] - mean


def gram_blocks(stack, extra, buffers, gram, blocks, m, r):
    sub = lax.broadcasted_iota(jnp.int32, (8, 128), 0)
    point_row = jnp.right_shift(sub, 2)
    center_row = (jnp.bitwise_and(jnp.right_shift(sub, 1), 1) * 8).astype(F32) + 3.5
    center_col = (jnp.bitwise_and(sub, 1) * 8).astype(F32) + 3.5
    zero = jnp.zeros((8, 128), F32)
    blank = jnp.zeros((16, 128), BF16)
    for n, (tr, c) in enumerate(blocks):
        lhs, loc = buffers[n // DEEP % 2]
        lanes = pl.ds(n % DEEP * 128, 128)
        cell = jnp.broadcast_to(extra[tr, 1, pl.ds(AT + c, 1), :], (8, 128)).astype(jnp.int32)
        cell_row = jnp.right_shift(cell, 4).astype(F32)
        cell_col = jnp.bitwise_and(cell, 15).astype(F32)
        row = r * ROWS + tr - 1
        column = m * COLS + c - 1
        inside = jnp.logical_and(jnp.logical_and(column >= 0, column < BCOLS), jnp.logical_and(row >= 0, row < BROWS))
        di = tr - 1 - point_row
        dy = (SIDE * di).astype(F32) + cell_row - center_row
        keep = jnp.logical_and(jnp.abs(di) <= 1, inside)
        reach = {}
        for e in (-1, 0, 1):
            if 0 <= c - 1 + e < COLS:
                dx = cell_col - center_col - float(SIDE * e)
                weight = jnp.exp((dy * dy + dx * dx) * (-1.0 / (2.0 * LOC_SCALE * LOC_SCALE)))
                reach[c - 1 + e] = jnp.where(keep, weight, 0.0)
        for tile in range(COLS // 2):
            if 2 * tile in reach or 2 * tile + 1 in reach:
                both = jnp.concatenate([reach.get(2 * tile, zero), reach.get(2 * tile + 1, zero)], axis=0)
                high = both.astype(BF16)
                low = (both - high.astype(F32)).astype(BF16)
            else:
                high = low = blank
            loc[pl.ds(16 * tile, 16), lanes] = high
            loc[pl.ds(128 + 16 * tile, 16), lanes] = low
        members = [stack[tr, c, pl.ds(8 * gj, 8), :] for gj in range(3)]
        turned = [[pltpu.roll(v, 8 - d, 0) if d else v for d in range(8)] for v in members]
        innovation = jnp.broadcast_to(extra[tr, 0, pl.ds(AT + c, 1), :], (8, 128))
        pieces = [members[ga] * turned[gb][d] for ga, gb, d in TERMS] + [innovation * v for v in members]
        for t in range(PAIRS // 16):
            both = jnp.concatenate(pieces[2 * t : 2 * t + 2], axis=0)
            high = both.astype(BF16)
            lhs[pl.ds(16 * t, 16), lanes] = high
            lhs[pl.ds(PAIRS + 16 * t, 16), lanes] = (both - high.astype(F32)).astype(BF16)
        if n % DEEP == DEEP - 1 or n == len(blocks) - 1:
            depth = pl.ds(0, 128 * (n % DEEP + 1))
            dims = (((1,), (1,)), ((), ()))
            high = lax.dot_general(lhs[pl.ds(0, PAIRS), depth], loc[:, depth], dims, preferred_element_type=F32)
            low = lax.dot_general(
                lhs[pl.ds(PAIRS, PAIRS), depth], loc[pl.ds(0, 128), depth], dims, preferred_element_type=F32
            )
            gram[...] = gram[...] + ((low + high[:, 128:]) + high[:, :128])


def update_members(x, means, wts, result, g, i, others):
    cols = pl.ds(pl.multiple_of(g * GROUP, GROUP), GROUP)
    sub = lax.broadcasted_iota(jnp.int32, (8, 128), 0)
    lane = lax.broadcasted_iota(jnp.int32, (8, 128), 1)
    base = (g * GROUP + sub) * 8 + i * 4 + jnp.bitwise_and(jnp.right_shift(lane, 3), 1)
    members = [other * MINE + u for other in others for u in range(MINE)]
    for h in range(2):
        index = base + 2 * h
        acc = [[means[i, cols, pl.ds(128 * (2 * f + h), 128)] for f in range(2)] for _ in members]
        for j in range(K):
            xs = [x[j, i, cols, pl.ds(128 * (2 * f + h), 128)] for f in range(2)]
            for u, k in enumerate(members):
                row = jnp.broadcast_to(wts[pl.ds(j * K + k, 1), :], (8, 128))
                wv = jnp.take_along_axis(row, index, axis=1, mode="promise_in_bounds")
                for f in range(2):
                    acc[u][f] = acc[u][f] + wv * xs[f]
        for u, k in enumerate(members):
            for f in range(2):
                result[k, i, cols, pl.ds(128 * (2 * f + h), 128)] = acc[u][f]


def kernel(
    ens, value_in, error_in, index_in, count_in, out,
    count,    value, error, index, load,
    x, obs, packed, stack, extra, means, lhs0, loc0, lhs1, loc1, mine, places, seen_out, seen, gram, wts, y, z, mm, tmp, rest, result,
    obs_send, obs_recv, in_send, in_recv, own_in, halo_send, halo_recv, out_send, out_recv, own_out, place_send, place_recv, seen_send, seen_recv,
):
    m = lax.axis_index("member")
    r = lax.axis_index("region")

    loads = [
        pltpu.make_async_copy(src, dst, load.at[n])
        for n, (src, dst) in enumerate(((value_in, value), (error_in, error), (index_in, index), (count_in, count), (ens, mine)))
    ]
    for copy in loads:
        copy.start()
    barrier = pltpu.get_barrier_semaphore()
    around = [dev(m + d, r) for d in range(1, NM)] + [dev(m, r + d) for d in range(1, NR)]
    around += [dev(m + a, r + b) for a in (-1, 1) for b in (-1, 1)]
    for device in around:
        pl.semaphore_signal(barrier, inc=1, device_id=device, device_id_type=MESH)
    for copy in loads[:4]:
        copy.wait()
    sub = lax.broadcasted_iota(jnp.int32, (8, OBS), 0)
    slot = lax.broadcasted_iota(jnp.int32, (8, OBS), 1)
    for n in range(BROWS // 8):
        rows = pl.ds(8 * n, 8)
        limit = jnp.zeros((8, OBS), jnp.int32)
        for u in range(8):
            limit = jnp.where(sub == u, count[0, 8 * n + u], limit)
        live = jnp.where(slot < limit, 1.0, 0.0).astype(F32)
        fields = (jnp.sqrt(live / error[rows, 0, :]), value[rows, 0, :], index[rows, 0, :].astype(F32))
        for f, field in enumerate(fields):
            for u in range(8):
                to = 8 * n + u
                packed[to // ROWS, to % ROWS * 4 + f, :] = field[u]
    pl.semaphore_wait(barrier, len(around))

    def obs_copy(d):
        other = lax.rem(r + d, NR)
        return remote(packed.at[other], obs.at[r], obs_send.at[0], obs_recv.at[0], (m, other))

    for d in range(1, NR):
        obs_copy(d).start()

    def in_copy(q, d):
        g, i = q // ROWS, q % ROWS
        other = lax.rem(m + d, NM)
        src = mine.at[:, i, pl.ds(pl.multiple_of(other * COLS + g * GROUP, GROUP), GROUP), :]
        dst = x.at[pl.ds(m * MINE, MINE), i, pl.ds(pl.multiple_of(g * GROUP, GROUP), GROUP), :]
        return remote(src, dst, in_send.at[q], in_recv.at[q], (other, r))

    def in_all(q):
        g, i = q // ROWS, q % ROWS
        part = x.at[pl.ds(0, K - MINE), i, pl.ds(pl.multiple_of(g * GROUP, GROUP), GROUP), :]
        return remote(part, part, in_send.at[q], in_recv.at[q], (m, r))

    def own_copy(q):
        g, i = q // ROWS, q % ROWS
        src = ens.at[:, i, pl.ds(pl.multiple_of(m * COLS + g * GROUP, GROUP), GROUP), :]
        dst = x.at[pl.ds(m * MINE, MINE), i, pl.ds(pl.multiple_of(g * GROUP, GROUP), GROUP), :]
        return pltpu.make_async_copy(src, dst, own_in.at[q])

    def send_in(q, part=range(NM)):
        for d in part:
            (in_copy(q, d) if d else own_copy(q)).start()

    loads[4].wait()
    send_in(0, (2, 6, 1, 7))
    obs[r] = packed[r]
    gram[...] = jnp.zeros_like(gram)
    obs_all = remote(packed.at[pl.ds(0, NR - 1)], obs.at[pl.ds(0, NR - 1)], obs_send.at[0], obs_recv.at[0], (m, r))
    obs_all.wait_recv()

    def place_copy(d):
        own = places.at[:, pl.ds(pl.multiple_of(m * COLS, COLS), COLS), :]
        return remote(own, own, place_send.at[0], place_recv.at[0], (lax.rem(m + d, NM), r))

    def seen_copy(g, d):
        other = lax.rem(m + d, NM)
        dst = seen.at[g, pl.ds(m * MINE, MINE)]
        return remote(seen_out.at[g, other], dst, seen_send.at[g], seen_recv.at[g], (other, r))

    def seen_all(g):
        part = seen.at[g, pl.ds(0, K - MINE)]
        return remote(part, part, seen_send.at[g], seen_recv.at[g], (m, r))

    for i in range(ROWS):
        for g in range(2):
            cols = pl.ds(pl.multiple_of(m * COLS + g * GROUP, GROUP), GROUP)
            places[i, cols, :] = obs[pl.ds(g * GROUP, GROUP), i * 4 + 2, :]
    for d in range(1, NM):
        place_copy(d).start()
    send_in(0, (3, 5, 4, 0))

    def halo_pair(src, dst, sem, device):
        return [remote(ref.at[a], ref.at[b], halo_send.at[sem], halo_recv.at[sem], device) for ref, a, b in zip((stack, extra), src, dst)]

    def row_halo(g, i):
        to = 3 if i == 0 else 0
        where, wide = pl.ds(1 + g * GROUP, GROUP), pl.ds((1 + g) * GROUP, GROUP)
        device = dev(m, r + (-1 if i == 0 else 1))
        return halo_pair(((1 + i, where), (1 + i, slice(None), wide)), ((to, where), (to, slice(None), wide)), ROWS * g + i, device)

    def side_halo(g):
        col, to, a = (1, COLS + 1, -1) if g == 0 else (COLS, 0, 1)
        wide, there = pl.ds((1 + g) * GROUP, GROUP), pl.ds((COLS + GROUP) * (1 - g), GROUP)
        copies = []
        for rows, to_rows, b in ((pl.ds(1, 2), pl.ds(1, 2), 0), (1, 3, -1), (2, 0, 1)):
            copies += halo_pair(
                ((rows, col), (rows, slice(None), wide)), ((to_rows, to), (to_rows, slice(None), there)), 4 + g, dev(m + a, r + b)
            )
        return copies

    def row_all(g, i):
        n = GROUP * K + 2 * GROUP
        return wait_for(n, ROWS * g + i)

    def side_all(g):
        return wait_for(4 * (K + 2 * GROUP), 4 + g)

    def wait_for(rows, sem):
        part = wts.at[pl.ds(0, rows), :]
        return remote(part, part, halo_send.at[sem], halo_recv.at[sem], (m, r))

    rest_of = places.at[:, pl.ds(0, BCOLS - COLS), :]
    place_all = remote(rest_of, rest_of, place_send.at[0], place_recv.at[0], (m, r))
    place_all.wait_recv()
    for g in range(2):
        gather_group(mine, places, seen_out, m, g)
        for d in range(1, NM):
            seen_copy(g, d).start()
        seen[g, pl.ds(m * MINE, MINE)] = seen_out[g, m]
    send_in(1)

    def arrive(g):
        seen_all(g).wait_recv()
        stack_group(seen, obs, stack, extra, g)
        for copy in row_halo(g, 0) + row_halo(g, 1) + side_halo(g):
            copy.start()

    def add(blocks):
        gram_blocks(stack, extra, ((lhs0, loc0), (lhs1, loc1)), gram, blocks, m, r)

    def own(g):
        return [(1 + i, 1 + g * GROUP + c) for i in range(ROWS) for c in range(GROUP)]

    def beyond(g):
        return [(3 * i, 1 + g * GROUP + c) for i in range(ROWS) for c in range(GROUP)]

    arrive(0)
    add(own(0))
    arrive(1)
    send_in(2)
    send_in(3)
    add(own(1))
    for i in range(ROWS):
        row_all(0, i).wait_recv()
    add(beyond(0))
    side_all(0).wait_recv()
    for i in range(ROWS):
        row_all(1, i).wait_recv()
    side_all(1).wait_recv()
    add(beyond(1) + [(tr, c) for tr in range(4) for c in (0, COLS + 1)])
    newton_schulz(gram, wts, y, z, mm, tmp, rest)

    def out_copy(q, d):
        g, i = q // ROWS, q % ROWS
        other = lax.rem(m + d, NM)
        src = result.at[pl.ds(other * MINE, MINE), i, pl.ds(pl.multiple_of(g * GROUP, GROUP), GROUP), :]
        dst = out.at[:, i, pl.ds(pl.multiple_of(m * COLS + g * GROUP, GROUP), GROUP), :]
        return remote(src, dst, out_send.at[q], out_recv.at[q], (other, r))

    def out_all(q):
        g, i = q // ROWS, q % ROWS
        part = result.at[pl.ds(0, K - MINE), i, pl.ds(pl.multiple_of(g * GROUP, GROUP), GROUP), :]
        return remote(part, part, out_send.at[q], out_recv.at[q], (m, r))

    def keep_copy(q):
        g, i = q // ROWS, q % ROWS
        src = result.at[pl.ds(m * MINE, MINE), i, pl.ds(pl.multiple_of(g * GROUP, GROUP), GROUP), :]
        dst = out.at[:, i, pl.ds(pl.multiple_of(m * COLS + g * GROUP, GROUP), GROUP), :]
        return pltpu.make_async_copy(src, dst, own_out.at[q])

    def chunk_out(q, carry):
        own_copy(q).wait()
        in_all(q).wait_recv()
        center_chunk(x, means, q // ROWS, q % ROWS)
        for pair in ((2, 6), (3, 5), (4, 1), (7, 0)):
            update_members(x, means, wts, result, q // ROWS, q % ROWS, [lax.rem(m + d, NM) for d in pair])
            for d in pair:
                (out_copy(q, d) if d else keep_copy(q)).start()
        return carry

    lax.fori_loop(0, len(CHUNKS), chunk_out, 0)

    obs_all.wait_send()
    place_all.wait_send()
    for g in range(2):
        seen_all(g).wait_send()
        side_all(g).wait_send()
        for i in range(ROWS):
            row_all(g, i).wait_send()
    for q in range(len(CHUNKS)):
        in_all(q).wait_send()
    for q in range(len(CHUNKS)):
        keep_copy(q).wait()
        out_all(q).wait_send()
        out_all(q).wait_recv()


def local(ensemble, obs_value, obs_error, obs_index, obs_count):
    dma = pltpu.SemaphoreType.DMA
    n = len(CHUNKS)
    square = pltpu.VMEM((K * K, 128), F32)
    hbm = [pltpu.with_memory_space_constraint(v, pltpu.MemorySpace.HBM) for v in (ensemble, obs_value, obs_error, obs_index, obs_count.reshape(1, BROWS))]
    return pl.pallas_call(
        kernel,
        out_shape=jax.ShapeDtypeStruct(ensemble.shape, F32),
        in_specs=[pl.BlockSpec(memory_space=pltpu.MemorySpace.HBM)] * 5,
        out_specs=pl.BlockSpec(memory_space=pl.ANY),
        scratch_shapes=[
            pltpu.SMEM((1, BROWS), jnp.int32),
            pltpu.VMEM((BROWS, 1, OBS), F32), pltpu.VMEM((BROWS, 1, OBS), F32), pltpu.VMEM((BROWS, 1, OBS), jnp.int32), dma((5,)),
            pltpu.VMEM((K, ROWS, COLS, VALS), F32),
            pltpu.VMEM((COLS, 4 * ROWS, OBS), F32),
            pltpu.VMEM((NR, 4 * ROWS, OBS), F32),
            pltpu.VMEM((ROWS + 2, COLS + 2, K, OBS), F32),
            pltpu.VMEM((ROWS + 2, 2, COLS + 2 * GROUP, OBS), F32),
            pltpu.VMEM((ROWS, COLS, VALS), F32),
            pltpu.VMEM((2 * PAIRS, DEEP * 128), BF16),
            pltpu.VMEM((256, DEEP * 128), BF16),
            pltpu.VMEM((2 * PAIRS, DEEP * 128), BF16),
            pltpu.VMEM((256, DEEP * 128), BF16),
            pltpu.VMEM((MINE, ROWS, BCOLS, VALS), F32),
            pltpu.VMEM((ROWS, BCOLS, OBS), F32),
            pltpu.VMEM((2, NM, MINE, ROWS, GROUP, OBS), F32),
            pltpu.VMEM((2, K, ROWS, GROUP, OBS), F32),
            pltpu.VMEM((PAIRS, 128), F32),
            square, square, square, square, square, square,
            pltpu.VMEM((K, ROWS, COLS, VALS), F32),
            dma((1,)), dma((1,)), dma((n,)), dma((n,)), dma((n,)),
            dma((6,)), dma((6,)), dma((n,)), dma((n,)), dma((n,)),
            dma((1,)), dma((1,)), dma((2,)), dma((2,)),
        ],
        compiler_params=pltpu.CompilerParams(collective_id=0, has_side_effects=True, vmem_limit_bytes=32 << 20),
    )(*hbm)


def solution(mesh):
    return jax.shard_map(
        local,
        mesh=mesh,
        in_specs=(
            P("member", "region", None, None),
            P(None, ("member", "region"), None),
            P(None, ("member", "region"), None),
            P(None, ("member", "region"), None),
            P(None, ("member", "region")),
        ),
        out_specs=P("member", "region", None, None),
        check_vma=False,
    )
```

```python
import functools
import math

import jax
import jax.numpy as jnp
from jax import lax
from jax.experimental import pallas as pl
from jax.experimental.pallas import tpu as pltpu
from jax.sharding import PartitionSpec as P

MESH = pl.DeviceIdType.MESH
F32 = jnp.float32
BF16 = jnp.bfloat16

SIDE = 16
OBS = 128
NS_ITERS = 6
VALS = 512
K = 24
BROWS = 32
BCOLS = 128
LOC_SCALE = 12.0
INFLATION_FACTOR = 1.1
NM = 8
NR = 16
MINE = K // NM
ROWS = BROWS // NR
COLS = BCOLS // NM
GROUP = 8
CHUNKS = [(g, i) for g in range(COLS // GROUP) for i in range(ROWS)]
AT = GROUP - 1
TERMS = [(a, b, d) for a in range(3) for b in range(a, 3) for d in range(8 if b > a else 5)]
DRIVE = 8 * len(TERMS)
PAIRS = DRIVE + K
DEEP = 8


def dev(m, r):
    return (lax.rem(m + NM, NM), lax.rem(r + NR, NR))


def remote(src, dst, send, recv, device):
    return pltpu.make_async_remote_copy(
        src_ref=src, dst_ref=dst, send_sem=send, recv_sem=recv, device_id=device, device_id_type=MESH
    )


def tri_product(dst, a, b, post):
    for ga, height in ((0, 4), (1, 4), (2, 8)):
        groups = list(range(ga, 3))
        for first in range(8 * ga, 8 * ga + 8, height):
            acc = [[None] * len(groups) for _ in range(height)]
            for k in range(K):
                bv = [b[pl.ds(k * K + 8 * gj, 8), :] for gj in groups]
                for u in range(height):
                    av = jnp.broadcast_to(a[pl.ds((first + u) * K + k, 1), :], (8, 128))
                    for n in range(len(groups)):
                        term = av * bv[n]
                        acc[u][n] = term if acc[u][n] is None else acc[u][n] + term
            for u in range(height):
                for n, gj in enumerate(groups):
                    dst[pl.ds((first + u) * K + 8 * gj, 8), :] = post(acc[u][n], first + u, gj)
    fill_lower(dst)


def fill_lower(dst):
    for i in range(8, K):
        for gj in range(i // 8):
            dst[pl.ds(i * K + 8 * gj, 8), :] = dst[pl.ds(8 * gj * K + i, 8, stride=K), :]


def unit(i, gj):
    if i // 8 != gj:
        return jnp.zeros((8, 128), F32)
    return jnp.where(lax.broadcasted_iota(jnp.int32, (8, 128), 0) == i % 8, 1.0, 0.0).astype(F32)


def same(v, i, gj):
    return v


def newton_schulz(gram, wts, p, s, t, z, rest):
    square = jnp.zeros((8, 128), F32)
    for ga in range(3):
        for gb in range(ga, 3):
            base = 8 * TERMS.index((ga, gb, 0))
            source, start = gram, base
            if ga == gb:
                source, start = rest, 64 * ga
                for d in range(8):
                    v = gram[pl.ds(base + 8 * min(d, 8 - d), 8), :]
                    rest[pl.ds(start + 8 * d, 8), :] = pltpu.roll(v, 8 - d, 0) if d > 4 else v
            for u in range(8):
                k = 8 * ga + u
                v = source[pl.ds(start + u, 8, stride=8), :]
                v = pltpu.roll(v, u, 0) if u else v
                if ga == gb:
                    v = v + (K - 1) / INFLATION_FACTOR * unit(k, gb)
                p[pl.ds(k * K + 8 * gb, 8), :] = v
                square = square + v * v * (1.0 if ga == gb else 2.0)
    norm = jnp.sqrt(jnp.sum(square, axis=0, keepdims=True))
    inv_norm = 1.0 / norm
    for k in range(K):
        for gj in range(k // 8, 3):
            rows = pl.ds(k * K + 8 * gj, 8)
            p[rows, :] = p[rows, :] * inv_norm
    fill_lower(p)

    def square_of(v, i, gj):
        rows = pl.ds(i * K + 8 * gj, 8)
        rest[rows, :] = 1.6875 * unit(i, gj) - 0.5625 * p[rows, :] + 0.0625 * v
        return v

    def factor_of(v, i, gj):
        return v + (2.25 * unit(i, gj) - 2.4375 * p[pl.ds(i * K + 8 * gj, 8), :])

    def factor(dst):
        tri_product(s, p, p, square_of)
        fill_lower(rest)
        tri_product(dst, s, rest, factor_of)

    factor(z)
    tri_product(t, p, z, same)
    tri_product(p, t, z, same)
    factor(t)
    tri_product(s, p, t, same)
    tri_product(p, s, t, same)
    tri_product(wts, z, t, same)
    factor(t)
    tri_product(z, wts, t, same)
    scale = 1.0 / jnp.sqrt(norm)

    def apply(vector):
        acc = [jnp.zeros((8, 128), F32) for _ in range(3)]
        for k in range(K):
            row = vector[k // 8][k % 8 : k % 8 + 1, :]
            for gj in range(3):
                acc[gj] = acc[gj] + z[pl.ds(k * K + 8 * gj, 8), :] * row
        return [v * scale for v in acc]

    drive = [gram[pl.ds(DRIVE + 8 * gj, 8), :] for gj in range(3)]
    mean_w = apply(apply(drive))
    root = scale * math.sqrt(K - 1)
    for j in range(K):
        row = mean_w[j // 8][j % 8 : j % 8 + 1, :]
        for gj in range(3):
            rows = pl.ds(j * K + 8 * gj, 8)
            wts[rows, :] = z[rows, :] * root + row


def gather_group(mine, places, seen_out, m, g):
    for other in range(NM):
        cols = pl.ds(other * COLS + g * GROUP, GROUP)
        for i in range(ROWS):
            index = places[i, cols, :].astype(jnp.int32)
            lane = jnp.bitwise_and(index, 127)
            tile = jnp.right_shift(index, 7)
            for u in range(MINE):
                v = [
                    jnp.take_along_axis(mine[u, i, cols, pl.ds(128 * t, 128)], lane, axis=1, mode="promise_in_bounds")
                    for t in range(4)
                ]
                low, high = jnp.where(tile < 1, v[0], v[1]), jnp.where(tile < 3, v[2], v[3])
                seen_out[g, other, u, i] = jnp.where(tile < 2, low, high)


def stack_group(seen, obs, stack, extra, g):
    cols = pl.ds(g * GROUP, GROUP)
    here = pl.ds(1 + g * GROUP, GROUP)
    for i in range(ROWS):
        total = seen[g, 0, i]
        for k in range(1, K):
            total = total + seen[g, k, i]
        mean = total * (1.0 / K)
        root_weight = obs[cols, i * 4 + 0, :]
        for k in range(K):
            stack[1 + i, here, k, :] = root_weight * (seen[g, k, i] - mean)
        index = obs[cols, i * 4 + 2, :].astype(jnp.int32)
        extra[1 + i, 0, pl.ds((1 + g) * GROUP, GROUP), :] = root_weight * (obs[cols, i * 4 + 1, :] - mean)
        extra[1 + i, 1, pl.ds((1 + g) * GROUP, GROUP), :] = jnp.bitwise_and(index, SIDE * SIDE - 1).astype(F32)


def center_chunk(x, means, g, i):
    cols = pl.ds(pl.multiple_of(g * GROUP, GROUP), GROUP)
    for t in range(4):
        lanes = pl.ds(128 * t, 128)
        total = x[0, i, cols, lanes]
        for k in range(1, K):
            total = total + x[k, i, cols, lanes]
        mean = total * (1.0 / K)
        means[i, cols, lanes] = mean
        for k in range(K):
            x[k, i, cols, lanes] = x[k, i, cols, lanes] - mean


def rounded(v):
    return v.astype(BF16).astype(F32)


def gram_blocks(stack, extra, buffers, gram, blocks, m, r):
    sub = lax.broadcasted_iota(jnp.int32, (8, 128), 0)
    point_row = jnp.right_shift(sub, 2)
    center_row = (jnp.bitwise_and(jnp.right_shift(sub, 1), 1) * 8).astype(F32) + 3.5
    center_col = (jnp.bitwise_and(sub, 1) * 8).astype(F32) + 3.5
    zero = jnp.zeros((8, 128), F32)
    for n, (tr, c) in enumerate(blocks):
        lhs, loc = buffers[n // DEEP % 2]
        lanes = pl.ds(n % DEEP * 128, 128)
        cell = jnp.broadcast_to(extra[tr, 1, pl.ds(AT + c, 1), :], (8, 128)).astype(jnp.int32)
        cell_row = jnp.right_shift(cell, 4).astype(F32)
        cell_col = jnp.bitwise_and(cell, 15).astype(F32)
        row = r * ROWS + tr - 1
        column = m * COLS + c - 1
        inside = jnp.logical_and(jnp.logical_and(column >= 0, column < BCOLS), jnp.logical_and(row >= 0, row < BROWS))
        di = tr - 1 - point_row
        dy = (SIDE * di).astype(F32) + cell_row - center_row
        keep = jnp.logical_and(jnp.abs(di) <= 1, inside)
        reach = {}
        for e in (-1, 0, 1):
            if 0 <= c - 1 + e < COLS:
                dx = cell_col - center_col - float(SIDE * e)
                weight = jnp.exp((dy * dy + dx * dx) * (-1.0 / (2.0 * LOC_SCALE * LOC_SCALE)))
                reach[c - 1 + e] = jnp.where(keep, weight, 0.0)
        for col in range(COLS):
            high = low = zero
            if col in reach:
                high = rounded(reach[col])
                low = reach[col] - high
            loc[pl.ds(8 * col, 8), lanes] = high
            loc[pl.ds(128 + 8 * col, 8), lanes] = low
        members = [stack[tr, c, pl.ds(8 * gj, 8), :] for gj in range(3)]
        turned = [[pltpu.roll(v, 8 - d, 0) if d else v for d in range(8)] for v in members]
        innovation = jnp.broadcast_to(extra[tr, 0, pl.ds(AT + c, 1), :], (8, 128))
        pieces = [members[ga] * turned[gb][d] for ga, gb, d in TERMS] + [innovation * v for v in members]
        for t in range(PAIRS // 16):
            both = jnp.concatenate(pieces[2 * t : 2 * t + 2], axis=0)
            lhs[pl.ds(16 * t, 16), lanes] = both
            lhs[pl.ds(PAIRS + 16 * t, 16), lanes] = both - rounded(both)
        if n % DEEP == DEEP - 1 or n == len(blocks) - 1:
            depth = pl.ds(0, 128 * (n % DEEP + 1))
            dims = (((1,), (1,)), ((), ()))
            high = lax.dot_general(lhs[pl.ds(0, PAIRS), depth], loc[:, depth], dims, precision=lax.Precision.DEFAULT, preferred_element_type=F32)
            low = lax.dot_general(
                lhs[pl.ds(PAIRS, PAIRS), depth], loc[pl.ds(0, 128), depth], dims, precision=lax.Precision.DEFAULT, preferred_element_type=F32
            )
            gram[...] = gram[...] + ((low + high[:, 128:]) + high[:, :128])


def update_members(x, means, wts, result, g, i, others):
    cols = pl.ds(pl.multiple_of(g * GROUP, GROUP), GROUP)
    sub = lax.broadcasted_iota(jnp.int32, (8, 128), 0)
    lane = lax.broadcasted_iota(jnp.int32, (8, 128), 1)
    base = (g * GROUP + sub) * 8 + i * 4 + jnp.bitwise_and(jnp.right_shift(lane, 3), 1)
    members = [other * MINE + u for other in others for u in range(MINE)]
    for h in range(2):
        index = base + 2 * h
        acc = [[means[i, cols, pl.ds(128 * (2 * f + h), 128)] for f in range(2)] for _ in members]
        for j in range(K):
            xs = [x[j, i, cols, pl.ds(128 * (2 * f + h), 128)] for f in range(2)]
            for u, k in enumerate(members):
                row = jnp.broadcast_to(wts[pl.ds(j * K + k, 1), :], (8, 128))
                wv = jnp.take_along_axis(row, index, axis=1, mode="promise_in_bounds")
                for f in range(2):
                    acc[u][f] = acc[u][f] + wv * xs[f]
        for u, k in enumerate(members):
            for f in range(2):
                result[k, i, cols, pl.ds(128 * (2 * f + h), 128)] = acc[u][f]


def kernel(
    ens, value_in, error_in, index_in, count_in, out,
    count,    value, error, index, load,
    x, obs, packed, stack, extra, means, lhs0, loc0, lhs1, loc1, mine, places, seen_out, seen, gram, wts, y, z, mm, tmp, rest, result,
    obs_send, obs_recv, in_send, in_recv, own_in, halo_send, halo_recv, out_send, out_recv, own_out, place_send, place_recv, seen_send, seen_recv,
):
    m = lax.axis_index("member")
    r = lax.axis_index("region")

    loads = [
        pltpu.make_async_copy(src, dst, load.at[n])
        for n, (src, dst) in enumerate(((value_in, value), (error_in, error), (index_in, index), (count_in, count), (ens, mine)))
    ]
    barrier = pltpu.get_barrier_semaphore()
    around = [dev(m + d, r) for d in range(1, NM)] + [dev(m, r + d) for d in range(1, NR)]
    around += [dev(m + a, r + b) for a in (-1, 1) for b in (-1, 1)]
    for device in around:
        pl.semaphore_signal(barrier, inc=1, device_id=device, device_id_type=MESH)
    for copy in loads:
        copy.start()
    for copy in loads[:4]:
        copy.wait()
    sub = lax.broadcasted_iota(jnp.int32, (8, OBS), 0)
    slot = lax.broadcasted_iota(jnp.int32, (8, OBS), 1)
    for n in range(BROWS // 8):
        rows = pl.ds(8 * n, 8)
        limit = jnp.zeros((8, OBS), jnp.int32)
        for u in range(8):
            limit = jnp.where(sub == u, count[0, 8 * n + u], limit)
        live = jnp.where(slot < limit, 1.0, 0.0).astype(F32)
        fields = (jnp.sqrt(live / error[rows, 0, :]), value[rows, 0, :], index[rows, 0, :].astype(F32))
        for f, field in enumerate(fields):
            for u in range(8):
                to = 8 * n + u
                packed[to // ROWS, to % ROWS * 4 + f, :] = field[u]
    pl.semaphore_wait(barrier, len(around))

    def obs_copy(d):
        other = lax.rem(r + d, NR)
        return remote(packed.at[other], obs.at[r], obs_send.at[0], obs_recv.at[0], (m, other))

    for d in range(1, NR):
        obs_copy(d).start()

    def in_copy(q, d):
        g, i = q // ROWS, q % ROWS
        other = lax.rem(m + d, NM)
        src = mine.at[:, i, pl.ds(pl.multiple_of(other * COLS + g * GROUP, GROUP), GROUP), :]
        dst = x.at[pl.ds(m * MINE, MINE), i, pl.ds(pl.multiple_of(g * GROUP, GROUP), GROUP), :]
        return remote(src, dst, in_send.at[q], in_recv.at[q], (other, r))

    def in_all(q):
        g, i = q // ROWS, q % ROWS
        part = x.at[pl.ds(0, K - MINE), i, pl.ds(pl.multiple_of(g * GROUP, GROUP), GROUP), :]
        return remote(part, part, in_send.at[q], in_recv.at[q], (m, r))

    def own_copy(q):
        g, i = q // ROWS, q % ROWS
        src = ens.at[:, i, pl.ds(pl.multiple_of(m * COLS + g * GROUP, GROUP), GROUP), :]
        dst = x.at[pl.ds(m * MINE, MINE), i, pl.ds(pl.multiple_of(g * GROUP, GROUP), GROUP), :]
        return pltpu.make_async_copy(src, dst, own_in.at[q])

    def send_in(q, part=range(NM)):
        for d in part:
            (in_copy(q, d) if d else own_copy(q)).start()

    loads[4].wait()
    send_in(0)
    obs[r] = packed[r]
    gram[...] = jnp.zeros_like(gram)
    obs_all = remote(packed.at[pl.ds(0, NR - 1)], obs.at[pl.ds(0, NR - 1)], obs_send.at[0], obs_recv.at[0], (m, r))
    obs_all.wait_recv()

    def place_copy(d):
        own = places.at[:, pl.ds(pl.multiple_of(m * COLS, COLS), COLS), :]
        return remote(own, own, place_send.at[0], place_recv.at[0], (lax.rem(m + d, NM), r))

    def seen_copy(g, d):
        other = lax.rem(m + d, NM)
        dst = seen.at[g, pl.ds(m * MINE, MINE)]
        return remote(seen_out.at[g, other], dst, seen_send.at[g], seen_recv.at[g], (other, r))

    def seen_all(g):
        part = seen.at[g, pl.ds(0, K - MINE)]
        return remote(part, part, seen_send.at[g], seen_recv.at[g], (m, r))

    for i in range(ROWS):
        for g in range(2):
            cols = pl.ds(pl.multiple_of(m * COLS + g * GROUP, GROUP), GROUP)
            places[i, cols, :] = obs[pl.ds(g * GROUP, GROUP), i * 4 + 2, :]
    for d in range(1, NM):
        place_copy(d).start()
    send_in(1, (2, 6, 1, 7, 3, 5, 0))

    def halo_pair(src, dst, sem, device):
        return [remote(ref.at[a], ref.at[b], halo_send.at[sem], halo_recv.at[sem], device) for ref, a, b in zip((stack, extra), src, dst)]

    def row_halo(g, i):
        to = 3 if i == 0 else 0
        where, wide = pl.ds(1 + g * GROUP, GROUP), pl.ds((1 + g) * GROUP, GROUP)
        device = dev(m, r + (-1 if i == 0 else 1))
        return halo_pair(((1 + i, where), (1 + i, slice(None), wide)), ((to, where), (to, slice(None), wide)), ROWS * g + i, device)

    def side_halo(g):
        col, to, a = (1, COLS + 1, -1) if g == 0 else (COLS, 0, 1)
        wide, there = pl.ds((1 + g) * GROUP, GROUP), pl.ds((COLS + GROUP) * (1 - g), GROUP)
        copies = []
        for rows, to_rows, b in ((pl.ds(1, 2), pl.ds(1, 2), 0), (1, 3, -1), (2, 0, 1)):
            copies += halo_pair(
                ((rows, col), (rows, slice(None), wide)), ((to_rows, to), (to_rows, slice(None), there)), 4 + g, dev(m + a, r + b)
            )
        return copies

    def row_all(g, i):
        n = GROUP * K + 2 * GROUP
        return wait_for(n, ROWS * g + i)

    def side_all(g):
        return wait_for(4 * (K + 2 * GROUP), 4 + g)

    def wait_for(rows, sem):
        part = wts.at[pl.ds(0, rows), :]
        return remote(part, part, halo_send.at[sem], halo_recv.at[sem], (m, r))

    rest_of = places.at[:, pl.ds(0, BCOLS - COLS), :]
    place_all = remote(rest_of, rest_of, place_send.at[0], place_recv.at[0], (m, r))
    place_all.wait_recv()
    for g in range(2):
        gather_group(mine, places, seen_out, m, g)
        for d in range(1, NM):
            seen_copy(g, d).start()
        seen[g, pl.ds(m * MINE, MINE)] = seen_out[g, m]

    def arrive(g):
        seen_all(g).wait_recv()
        stack_group(seen, obs, stack, extra, g)
        for copy in side_halo(g) + row_halo(g, 0) + row_halo(g, 1):
            copy.start()

    def add(blocks):
        gram_blocks(stack, extra, ((lhs0, loc0), (lhs1, loc1)), gram, blocks, m, r)

    def own(g):
        return [(1 + i, 1 + g * GROUP + c) for i in range(ROWS) for c in range(GROUP)]

    def beyond(g):
        return [(3 * i, 1 + g * GROUP + c) for i in range(ROWS) for c in range(GROUP)]

    arrive(0)
    send_in(1, (4,))
    send_in(2, (2, 6, 1, 7))
    add(own(0))
    arrive(1)
    send_in(2, (3, 5, 4, 0))
    send_in(3)
    add(own(1))
    for i in range(ROWS):
        row_all(0, i).wait_recv()
    add(beyond(0))
    side_all(0).wait_recv()
    add([(tr, COLS + 1) for tr in range(4)])
    for i in range(ROWS):
        row_all(1, i).wait_recv()
    side_all(1).wait_recv()
    add(beyond(1) + [(tr, 0) for tr in range(4)])
    newton_schulz(gram, wts, y, z, mm, tmp, rest)

    def out_copy(q, d):
        g, i = q // ROWS, q % ROWS
        other = lax.rem(m + d, NM)
        src = result.at[pl.ds(other * MINE, MINE), i, pl.ds(pl.multiple_of(g * GROUP, GROUP), GROUP), :]
        dst = out.at[:, i, pl.ds(pl.multiple_of(m * COLS + g * GROUP, GROUP), GROUP), :]
        return remote(src, dst, out_send.at[q], out_recv.at[q], (other, r))

    def out_all(q):
        g, i = q // ROWS, q % ROWS
        part = result.at[pl.ds(0, K - MINE), i, pl.ds(pl.multiple_of(g * GROUP, GROUP), GROUP), :]
        return remote(part, part, out_send.at[q], out_recv.at[q], (m, r))

    def keep_copy(q):
        g, i = q // ROWS, q % ROWS
        src = result.at[pl.ds(m * MINE, MINE), i, pl.ds(pl.multiple_of(g * GROUP, GROUP), GROUP), :]
        dst = out.at[:, i, pl.ds(pl.multiple_of(m * COLS + g * GROUP, GROUP), GROUP), :]
        return pltpu.make_async_copy(src, dst, own_out.at[q])

    def chunk_out(q, carry):
        own_copy(q).wait()
        in_all(q).wait_recv()
        center_chunk(x, means, q // ROWS, q % ROWS)
        for pair in ((2, 6), (3, 5), (4, 1), (7, 0)):
            update_members(x, means, wts, result, q // ROWS, q % ROWS, [lax.rem(m + d, NM) for d in pair])
            for d in pair:
                (out_copy(q, d) if d else keep_copy(q)).start()
        return carry

    lax.fori_loop(0, len(CHUNKS), chunk_out, 0)

    obs_all.wait_send()
    place_all.wait_send()
    for g in range(2):
        seen_all(g).wait_send()
        side_all(g).wait_send()
        for i in range(ROWS):
            row_all(g, i).wait_send()
    for q in range(len(CHUNKS)):
        in_all(q).wait_send()
    for q in range(len(CHUNKS)):
        keep_copy(q).wait()
        out_all(q).wait_send()
        out_all(q).wait_recv()


def local(ensemble, obs_value, obs_error, obs_index, obs_count):
    dma = pltpu.SemaphoreType.DMA
    n = len(CHUNKS)
    square = pltpu.VMEM((K * K, 128), F32)
    hbm = [pltpu.with_memory_space_constraint(v, pltpu.MemorySpace.HBM) for v in (ensemble, obs_value, obs_error, obs_index, obs_count.reshape(1, BROWS))]
    return pl.pallas_call(
        kernel,
        out_shape=jax.ShapeDtypeStruct(ensemble.shape, F32),
        in_specs=[pl.BlockSpec(memory_space=pltpu.MemorySpace.HBM)] * 5,
        out_specs=pl.BlockSpec(memory_space=pl.ANY),
        scratch_shapes=[
            pltpu.SMEM((1, BROWS), jnp.int32),
            pltpu.VMEM((BROWS, 1, OBS), F32), pltpu.VMEM((BROWS, 1, OBS), F32), pltpu.VMEM((BROWS, 1, OBS), jnp.int32), dma((5,)),
            pltpu.VMEM((K, ROWS, COLS, VALS), F32),
            pltpu.VMEM((COLS, 4 * ROWS, OBS), F32),
            pltpu.VMEM((NR, 4 * ROWS, OBS), F32),
            pltpu.VMEM((ROWS + 2, COLS + 2, K, OBS), F32),
            pltpu.VMEM((ROWS + 2, 2, COLS + 2 * GROUP, OBS), F32),
            pltpu.VMEM((ROWS, COLS, VALS), F32),
            pltpu.VMEM((2 * PAIRS, DEEP * 128), F32),
            pltpu.VMEM((256, DEEP * 128), F32),
            pltpu.VMEM((2 * PAIRS, DEEP * 128), F32),
            pltpu.VMEM((256, DEEP * 128), F32),
            pltpu.VMEM((MINE, ROWS, BCOLS, VALS), F32),
            pltpu.VMEM((ROWS, BCOLS, OBS), F32),
            pltpu.VMEM((2, NM, MINE, ROWS, GROUP, OBS), F32),
            pltpu.VMEM((2, K, ROWS, GROUP, OBS), F32),
            pltpu.VMEM((PAIRS, 128), F32),
            square, square, square, square, square, square,
            pltpu.VMEM((K, ROWS, COLS, VALS), F32),
            dma((1,)), dma((1,)), dma((n,)), dma((n,)), dma((n,)),
            dma((6,)), dma((6,)), dma((n,)), dma((n,)), dma((n,)),
            dma((1,)), dma((1,)), dma((2,)), dma((2,)),
        ],
        compiler_params=pltpu.CompilerParams(collective_id=0, has_side_effects=True, vmem_limit_bytes=40 << 20),
    )(*hbm)


def solution(mesh):
    return jax.shard_map(
        local,
        mesh=mesh,
        in_specs=(
            P("member", "region", None, None),
            P(None, ("member", "region"), None),
            P(None, ("member", "region"), None),
            P(None, ("member", "region"), None),
            P(None, ("member", "region")),
        ),
        out_specs=P("member", "region", None, None),
        check_vma=False,
    )
```

```python
import functools
import math

import jax
import jax.numpy as jnp
from jax import lax
from jax.experimental import pallas as pl
from jax.experimental.pallas import tpu as pltpu
from jax.sharding import PartitionSpec as P

MESH = pl.DeviceIdType.MESH
F32 = jnp.float32
BF16 = jnp.bfloat16

SIDE = 16
OBS = 128
NS_ITERS = 6
VALS = 512
K = 24
BROWS = 32
BCOLS = 128
LOC_SCALE = 12.0
INFLATION_FACTOR = 1.1
NM = 8
NR = 16
MINE = K // NM
ROWS = BROWS // NR
COLS = BCOLS // NM
GROUP = 8
CHUNKS = [(g, i) for g in range(COLS // GROUP) for i in range(ROWS)]
AT = GROUP - 1
TERMS = [(a, b, d) for a in range(3) for b in range(a, 3) for d in range(8 if b > a else 5)]
DRIVE = 8 * len(TERMS)
PAIRS = DRIVE + K
DEEP = 8


def dev(m, r):
    return (lax.rem(m + NM, NM), lax.rem(r + NR, NR))


def remote(src, dst, send, recv, device):
    return pltpu.make_async_remote_copy(
        src_ref=src, dst_ref=dst, send_sem=send, recv_sem=recv, device_id=device, device_id_type=MESH
    )


def tri_product(dst, a, b, post):
    for ga, height in ((0, 4), (1, 4), (2, 8)):
        groups = list(range(ga, 3))
        for first in range(8 * ga, 8 * ga + 8, height):
            acc = [[None] * len(groups) for _ in range(height)]
            for k in range(K):
                bv = [b[pl.ds(k * K + 8 * gj, 8), :] for gj in groups]
                for u in range(height):
                    av = jnp.broadcast_to(a[pl.ds((first + u) * K + k, 1), :], (8, 128))
                    for n in range(len(groups)):
                        term = av * bv[n]
                        acc[u][n] = term if acc[u][n] is None else acc[u][n] + term
            for u in range(height):
                for n, gj in enumerate(groups):
                    dst[pl.ds((first + u) * K + 8 * gj, 8), :] = post(acc[u][n], first + u, gj)
    fill_lower(dst)


def fill_lower(dst):
    for i in range(8, K):
        for gj in range(i // 8):
            dst[pl.ds(i * K + 8 * gj, 8), :] = dst[pl.ds(8 * gj * K + i, 8, stride=K), :]


def unit(i, gj):
    if i // 8 != gj:
        return jnp.zeros((8, 128), F32)
    return jnp.where(lax.broadcasted_iota(jnp.int32, (8, 128), 0) == i % 8, 1.0, 0.0).astype(F32)


def same(v, i, gj):
    return v


def newton_schulz(gram, wts, p, s, t, z, rest):
    square = jnp.zeros((8, 128), F32)
    for ga in range(3):
        for gb in range(ga, 3):
            base = 8 * TERMS.index((ga, gb, 0))
            source, start = gram, base
            if ga == gb:
                source, start = rest, 64 * ga
                for d in range(8):
                    v = gram[pl.ds(base + 8 * min(d, 8 - d), 8), :]
                    rest[pl.ds(start + 8 * d, 8), :] = pltpu.roll(v, 8 - d, 0) if d > 4 else v
            for u in range(8):
                k = 8 * ga + u
                v = source[pl.ds(start + u, 8, stride=8), :]
                v = pltpu.roll(v, u, 0) if u else v
                if ga == gb:
                    v = v + (K - 1) / INFLATION_FACTOR * unit(k, gb)
                p[pl.ds(k * K + 8 * gb, 8), :] = v
                square = square + v * v * (1.0 if ga == gb else 2.0)
    norm = jnp.sqrt(jnp.sum(square, axis=0, keepdims=True))
    inv_norm = 1.0 / norm
    for k in range(K):
        for gj in range(k // 8, 3):
            rows = pl.ds(k * K + 8 * gj, 8)
            p[rows, :] = p[rows, :] * inv_norm
    fill_lower(p)

    def square_of(v, i, gj):
        rows = pl.ds(i * K + 8 * gj, 8)
        rest[rows, :] = 1.6875 * unit(i, gj) - 0.5625 * p[rows, :] + 0.0625 * v
        return v

    def factor_of(v, i, gj):
        return v + (2.25 * unit(i, gj) - 2.4375 * p[pl.ds(i * K + 8 * gj, 8), :])

    def factor(dst):
        tri_product(s, p, p, square_of)
        fill_lower(rest)
        tri_product(dst, s, rest, factor_of)

    factor(z)
    tri_product(t, p, z, same)
    tri_product(p, t, z, same)
    factor(t)
    tri_product(s, p, t, same)
    tri_product(p, s, t, same)
    tri_product(wts, z, t, same)
    factor(t)
    tri_product(z, wts, t, same)
    scale = 1.0 / jnp.sqrt(norm)

    def apply(vector):
        acc = [jnp.zeros((8, 128), F32) for _ in range(3)]
        for k in range(K):
            row = vector[k // 8][k % 8 : k % 8 + 1, :]
            for gj in range(3):
                acc[gj] = acc[gj] + z[pl.ds(k * K + 8 * gj, 8), :] * row
        return [v * scale for v in acc]

    drive = [gram[pl.ds(DRIVE + 8 * gj, 8), :] for gj in range(3)]
    mean_w = apply(apply(drive))
    root = scale * math.sqrt(K - 1)
    for j in range(K):
        row = mean_w[j // 8][j % 8 : j % 8 + 1, :]
        for gj in range(3):
            rows = pl.ds(j * K + 8 * gj, 8)
            wts[rows, :] = z[rows, :] * root + row


def gather_group(mine, places, seen_out, m, g):
    for other in range(NM):
        cols = pl.ds(other * COLS + g * GROUP, GROUP)
        for i in range(ROWS):
            index = places[i, cols, :].astype(jnp.int32)
            lane = jnp.bitwise_and(index, 127)
            tile = jnp.right_shift(index, 7)
            for u in range(MINE):
                v = [
                    jnp.take_along_axis(mine[u, i, cols, pl.ds(128 * t, 128)], lane, axis=1, mode="promise_in_bounds")
                    for t in range(4)
                ]
                low, high = jnp.where(tile < 1, v[0], v[1]), jnp.where(tile < 3, v[2], v[3])
                seen_out[g, other, u, i] = jnp.where(tile < 2, low, high)


def stack_chunk(x, obs, stack, extra, means, i):
    cols = pl.ds(0, GROUP)
    center_chunk(x, means, 0, i)
    root_weight = obs[cols, i * 4 + 0, :]
    index = obs[cols, i * 4 + 2, :].astype(jnp.int32)
    lane = jnp.bitwise_and(index, 127)
    tile = jnp.right_shift(index, 7)

    def pick(ref):
        v = [
            jnp.take_along_axis(ref[i, cols, pl.ds(128 * t, 128)], lane, axis=1, mode="promise_in_bounds")
            for t in range(4)
        ]
        low, high = jnp.where(tile < 1, v[0], v[1]), jnp.where(tile < 3, v[2], v[3])
        return jnp.where(tile < 2, low, high)

    for k in range(K):
        stack[1 + i, pl.ds(1, GROUP), k, :] = root_weight * pick(x.at[k])
    extra[1 + i, 0, pl.ds(GROUP, GROUP), :] = root_weight * (obs[cols, i * 4 + 1, :] - pick(means))
    extra[1 + i, 1, pl.ds(GROUP, GROUP), :] = jnp.bitwise_and(index, SIDE * SIDE - 1).astype(F32)


def stack_group(seen, obs, stack, extra, g):
    cols = pl.ds(g * GROUP, GROUP)
    here = pl.ds(1 + g * GROUP, GROUP)
    for i in range(ROWS):
        total = seen[g, 0, i]
        for k in range(1, K):
            total = total + seen[g, k, i]
        mean = total * (1.0 / K)
        root_weight = obs[cols, i * 4 + 0, :]
        for k in range(K):
            stack[1 + i, here, k, :] = root_weight * (seen[g, k, i] - mean)
        index = obs[cols, i * 4 + 2, :].astype(jnp.int32)
        extra[1 + i, 0, pl.ds((1 + g) * GROUP, GROUP), :] = root_weight * (obs[cols, i * 4 + 1, :] - mean)
        extra[1 + i, 1, pl.ds((1 + g) * GROUP, GROUP), :] = jnp.bitwise_and(index, SIDE * SIDE - 1).astype(F32)


def center_chunk(x, means, g, i):
    cols = pl.ds(pl.multiple_of(g * GROUP, GROUP), GROUP)
    for t in range(4):
        lanes = pl.ds(128 * t, 128)
        total = x[0, i, cols, lanes]
        for k in range(1, K):
            total = total + x[k, i, cols, lanes]
        mean = total * (1.0 / K)
        means[i, cols, lanes] = mean
        for k in range(K):
            x[k, i, cols, lanes] = x[k, i, cols, lanes] - mean


def rounded(v):
    return v.astype(BF16).astype(F32)


def gram_blocks(stack, extra, buffers, gram, blocks, m, r):
    sub = lax.broadcasted_iota(jnp.int32, (8, 128), 0)
    point_row = jnp.right_shift(sub, 2)
    center_row = (jnp.bitwise_and(jnp.right_shift(sub, 1), 1) * 8).astype(F32) + 3.5
    center_col = (jnp.bitwise_and(sub, 1) * 8).astype(F32) + 3.5
    zero = jnp.zeros((8, 128), F32)
    for n, (tr, c) in enumerate(blocks):
        lhs, loc = buffers[n // DEEP % 2]
        lanes = pl.ds(n % DEEP * 128, 128)
        cell = jnp.broadcast_to(extra[tr, 1, pl.ds(AT + c, 1), :], (8, 128)).astype(jnp.int32)
        cell_row = jnp.right_shift(cell, 4).astype(F32)
        cell_col = jnp.bitwise_and(cell, 15).astype(F32)
        row = r * ROWS + tr - 1
        column = m * COLS + c - 1
        inside = jnp.logical_and(jnp.logical_and(column >= 0, column < BCOLS), jnp.logical_and(row >= 0, row < BROWS))
        di = tr - 1 - point_row
        dy = (SIDE * di).astype(F32) + cell_row - center_row
        keep = jnp.logical_and(jnp.abs(di) <= 1, inside)
        reach = {}
        for e in (-1, 0, 1):
            if 0 <= c - 1 + e < COLS:
                dx = cell_col - center_col - float(SIDE * e)
                weight = jnp.exp((dy * dy + dx * dx) * (-1.0 / (2.0 * LOC_SCALE * LOC_SCALE)))
                reach[c - 1 + e] = jnp.where(keep, weight, 0.0)
        for col in range(COLS):
            high = low = zero
            if col in reach:
                high = rounded(reach[col])
                low = reach[col] - high
            loc[pl.ds(8 * col, 8), lanes] = high
            loc[pl.ds(128 + 8 * col, 8), lanes] = low
        members = [stack[tr, c, pl.ds(8 * gj, 8), :] for gj in range(3)]
        turned = [[pltpu.roll(v, 8 - d, 0) if d else v for d in range(8)] for v in members]
        innovation = jnp.broadcast_to(extra[tr, 0, pl.ds(AT + c, 1), :], (8, 128))
        pieces = [members[ga] * turned[gb][d] for ga, gb, d in TERMS] + [innovation * v for v in members]
        for t in range(PAIRS // 16):
            both = jnp.concatenate(pieces[2 * t : 2 * t + 2], axis=0)
            lhs[pl.ds(16 * t, 16), lanes] = both
            lhs[pl.ds(PAIRS + 16 * t, 16), lanes] = both - rounded(both)
        if n % DEEP == DEEP - 1 or n == len(blocks) - 1:
            depth = pl.ds(0, 128 * (n % DEEP + 1))
            dims = (((1,), (1,)), ((), ()))
            high = lax.dot_general(lhs[pl.ds(0, PAIRS), depth], loc[:, depth], dims, precision=lax.Precision.DEFAULT, preferred_element_type=F32)
            low = lax.dot_general(
                lhs[pl.ds(PAIRS, PAIRS), depth], loc[pl.ds(0, 128), depth], dims, precision=lax.Precision.DEFAULT, preferred_element_type=F32
            )
            gram[...] = gram[...] + ((low + high[:, 128:]) + high[:, :128])


def update_members(x, means, wts, result, g, i, others):
    cols = pl.ds(pl.multiple_of(g * GROUP, GROUP), GROUP)
    sub = lax.broadcasted_iota(jnp.int32, (8, 128), 0)
    lane = lax.broadcasted_iota(jnp.int32, (8, 128), 1)
    base = (g * GROUP + sub) * 8 + i * 4 + jnp.bitwise_and(jnp.right_shift(lane, 3), 1)
    members = [other * MINE + u for other in others for u in range(MINE)]
    for h in range(2):
        index = base + 2 * h
        acc = [[means[i, cols, pl.ds(128 * (2 * f + h), 128)] for f in range(2)] for _ in members]
        for j in range(K):
            xs = [x[j, i, cols, pl.ds(128 * (2 * f + h), 128)] for f in range(2)]
            for u, k in enumerate(members):
                row = jnp.broadcast_to(wts[pl.ds(j * K + k, 1), :], (8, 128))
                wv = jnp.take_along_axis(row, index, axis=1, mode="promise_in_bounds")
                for f in range(2):
                    acc[u][f] = acc[u][f] + wv * xs[f]
        for u, k in enumerate(members):
            for f in range(2):
                result[k, i, cols, pl.ds(128 * (2 * f + h), 128)] = acc[u][f]


def kernel(
    ens, value_in, error_in, index_in, count_in, out,
    count,    value, error, index, load,
    x, obs, packed, stack, extra, means, lhs0, loc0, lhs1, loc1, mine, places, seen_out, seen, gram, wts, y, z, mm, tmp, rest, result,
    obs_send, obs_recv, in_send, in_recv, own_in, halo_send, halo_recv, out_send, out_recv, own_out, place_send, place_recv, seen_send, seen_recv,
):
    m = lax.axis_index("member")
    r = lax.axis_index("region")

    loads = [
        pltpu.make_async_copy(src, dst, load.at[n])
        for n, (src, dst) in enumerate(((value_in, value), (error_in, error), (index_in, index), (count_in, count), (ens, mine)))
    ]
    barrier = pltpu.get_barrier_semaphore()
    around = [dev(m + d, r) for d in range(1, NM)] + [dev(m, r + d) for d in range(1, NR)]
    around += [dev(m + a, r + b) for a in (-1, 1) for b in (-1, 1)]
    for device in around:
        pl.semaphore_signal(barrier, inc=1, device_id=device, device_id_type=MESH)
    for copy in loads:
        copy.start()
    for copy in loads[:4]:
        copy.wait()
    sub = lax.broadcasted_iota(jnp.int32, (8, OBS), 0)
    slot = lax.broadcasted_iota(jnp.int32, (8, OBS), 1)
    for n in range(BROWS // 8):
        rows = pl.ds(8 * n, 8)
        limit = jnp.zeros((8, OBS), jnp.int32)
        for u in range(8):
            limit = jnp.where(sub == u, count[0, 8 * n + u], limit)
        live = jnp.where(slot < limit, 1.0, 0.0).astype(F32)
        fields = (jnp.sqrt(live / error[rows, 0, :]), value[rows, 0, :], index[rows, 0, :].astype(F32))
        for f, field in enumerate(fields):
            for u in range(8):
                to = 8 * n + u
                packed[to // ROWS, to % ROWS * 4 + f, :] = field[u]
    pl.semaphore_wait(barrier, len(around))

    def obs_copy(d):
        other = lax.rem(r + d, NR)
        return remote(packed.at[other], obs.at[r], obs_send.at[0], obs_recv.at[0], (m, other))

    for d in range(1, NR):
        obs_copy(d).start()

    def in_copy(q, d):
        g, i = q // ROWS, q % ROWS
        other = lax.rem(m + d, NM)
        src = mine.at[:, i, pl.ds(pl.multiple_of(other * COLS + g * GROUP, GROUP), GROUP), :]
        dst = x.at[pl.ds(m * MINE, MINE), i, pl.ds(pl.multiple_of(g * GROUP, GROUP), GROUP), :]
        return remote(src, dst, in_send.at[q], in_recv.at[q], (other, r))

    def in_all(q):
        g, i = q // ROWS, q % ROWS
        part = x.at[pl.ds(0, K - MINE), i, pl.ds(pl.multiple_of(g * GROUP, GROUP), GROUP), :]
        return remote(part, part, in_send.at[q], in_recv.at[q], (m, r))

    def own_copy(q):
        g, i = q // ROWS, q % ROWS
        src = ens.at[:, i, pl.ds(pl.multiple_of(m * COLS + g * GROUP, GROUP), GROUP), :]
        dst = x.at[pl.ds(m * MINE, MINE), i, pl.ds(pl.multiple_of(g * GROUP, GROUP), GROUP), :]
        return pltpu.make_async_copy(src, dst, own_in.at[q])

    def send_in(q, part=range(NM)):
        for d in part:
            (in_copy(q, d) if d else own_copy(q)).start()

    loads[4].wait()
    send_in(0)
    obs[r] = packed[r]
    gram[...] = jnp.zeros_like(gram)
    obs_all = remote(packed.at[pl.ds(0, NR - 1)], obs.at[pl.ds(0, NR - 1)], obs_send.at[0], obs_recv.at[0], (m, r))
    obs_all.wait_recv()

    def place_copy(d):
        own = places.at[:, pl.ds(pl.multiple_of(m * COLS + GROUP, GROUP), GROUP), :]
        return remote(own, own, place_send.at[0], place_recv.at[0], (lax.rem(m + d, NM), r))

    def seen_copy(g, d):
        other = lax.rem(m + d, NM)
        dst = seen.at[g, pl.ds(m * MINE, MINE)]
        return remote(seen_out.at[g, other], dst, seen_send.at[g], seen_recv.at[g], (other, r))

    def seen_all(g):
        part = seen.at[g, pl.ds(0, K - MINE)]
        return remote(part, part, seen_send.at[g], seen_recv.at[g], (m, r))

    for i in range(ROWS):
        cols = pl.ds(pl.multiple_of(m * COLS + GROUP, GROUP), GROUP)
        places[i, cols, :] = obs[pl.ds(GROUP, GROUP), i * 4 + 2, :]
    for d in range(1, NM):
        place_copy(d).start()
    send_in(1)

    def halo_pair(src, dst, sem, device):
        return [remote(ref.at[a], ref.at[b], halo_send.at[sem], halo_recv.at[sem], device) for ref, a, b in zip((stack, extra), src, dst)]

    def row_halo(g, i):
        to = 3 if i == 0 else 0
        where, wide = pl.ds(1 + g * GROUP, GROUP), pl.ds((1 + g) * GROUP, GROUP)
        device = dev(m, r + (-1 if i == 0 else 1))
        return halo_pair(((1 + i, where), (1 + i, slice(None), wide)), ((to, where), (to, slice(None), wide)), ROWS * g + i, device)

    def side_halo(g):
        col, to, a = (1, COLS + 1, -1) if g == 0 else (COLS, 0, 1)
        wide, there = pl.ds((1 + g) * GROUP, GROUP), pl.ds((COLS + GROUP) * (1 - g), GROUP)
        copies = []
        for rows, to_rows, b in ((pl.ds(1, 2), pl.ds(1, 2), 0), (1, 3, -1), (2, 0, 1)):
            copies += halo_pair(
                ((rows, col), (rows, slice(None), wide)), ((to_rows, to), (to_rows, slice(None), there)), 4 + g, dev(m + a, r + b)
            )
        return copies

    def row_all(g, i):
        n = GROUP * K + 2 * GROUP
        return wait_for(n, ROWS * g + i)

    def side_all(g):
        return wait_for(4 * (K + 2 * GROUP), 4 + g)

    def wait_for(rows, sem):
        part = wts.at[pl.ds(0, rows), :]
        return remote(part, part, halo_send.at[sem], halo_recv.at[sem], (m, r))

    def arrive(i):
        own_copy(i).wait()
        in_all(i).wait_recv()
        stack_chunk(x, obs, stack, extra, means, i)

    arrive(0)
    for copy in row_halo(0, 0):
        copy.start()
    rest_of = places.at[:, pl.ds(0, (NM - 1) * GROUP), :]
    place_all = remote(rest_of, rest_of, place_send.at[0], place_recv.at[0], (m, r))
    place_all.wait_recv()
    gather_group(mine, places, seen_out, m, 1)
    for d in range(1, NM):
        seen_copy(1, d).start()
    seen[1, pl.ds(m * MINE, MINE)] = seen_out[1, m]

    def add(blocks):
        gram_blocks(stack, extra, ((lhs0, loc0), (lhs1, loc1)), gram, blocks, m, r)

    def own(g):
        return [(1 + i, 1 + g * GROUP + c) for i in range(ROWS) for c in range(GROUP)]

    def beyond(g):
        return [(3 * i, 1 + g * GROUP + c) for i in range(ROWS) for c in range(GROUP)]

    arrive(1)
    for copy in side_halo(0) + row_halo(0, 1):
        copy.start()
    send_in(2, (2, 6, 1, 7))
    add(own(0))
    seen_all(1).wait_recv()
    stack_group(seen, obs, stack, extra, 1)
    for copy in side_halo(1) + row_halo(1, 0) + row_halo(1, 1):
        copy.start()
    send_in(2, (3, 5, 4, 0))
    send_in(3)
    add(own(1))
    for i in range(ROWS):
        row_all(0, i).wait_recv()
    add(beyond(0))
    side_all(0).wait_recv()
    add([(tr, COLS + 1) for tr in range(4)])
    for i in range(ROWS):
        row_all(1, i).wait_recv()
    side_all(1).wait_recv()
    add(beyond(1) + [(tr, 0) for tr in range(4)])
    newton_schulz(gram, wts, y, z, mm, tmp, rest)

    def out_copy(q, d):
        g, i = q // ROWS, q % ROWS
        other = lax.rem(m + d, NM)
        src = result.at[pl.ds(other * MINE, MINE), i, pl.ds(pl.multiple_of(g * GROUP, GROUP), GROUP), :]
        dst = out.at[:, i, pl.ds(pl.multiple_of(m * COLS + g * GROUP, GROUP), GROUP), :]
        return remote(src, dst, out_send.at[q], out_recv.at[q], (other, r))

    def out_all(q):
        g, i = q // ROWS, q % ROWS
        part = result.at[pl.ds(0, K - MINE), i, pl.ds(pl.multiple_of(g * GROUP, GROUP), GROUP), :]
        return remote(part, part, out_send.at[q], out_recv.at[q], (m, r))

    def keep_copy(q):
        g, i = q // ROWS, q % ROWS
        src = result.at[pl.ds(m * MINE, MINE), i, pl.ds(pl.multiple_of(g * GROUP, GROUP), GROUP), :]
        dst = out.at[:, i, pl.ds(pl.multiple_of(m * COLS + g * GROUP, GROUP), GROUP), :]
        return pltpu.make_async_copy(src, dst, own_out.at[q])

    def chunk_out(q, carry):
        @pl.when(q >= ROWS)
        def _():
            own_copy(q).wait()
            in_all(q).wait_recv()
            center_chunk(x, means, q // ROWS, q % ROWS)

        for pair in ((2, 6), (3, 5), (4, 1), (7, 0)):
            update_members(x, means, wts, result, q // ROWS, q % ROWS, [lax.rem(m + d, NM) for d in pair])
            for d in pair:
                (out_copy(q, d) if d else keep_copy(q)).start()
        return carry

    lax.fori_loop(0, len(CHUNKS), chunk_out, 0)

    obs_all.wait_send()
    place_all.wait_send()
    seen_all(1).wait_send()
    for g in range(2):
        side_all(g).wait_send()
        for i in range(ROWS):
            row_all(g, i).wait_send()
    for q in range(len(CHUNKS)):
        in_all(q).wait_send()
    for q in range(len(CHUNKS)):
        keep_copy(q).wait()
        out_all(q).wait_send()
        out_all(q).wait_recv()


def local(ensemble, obs_value, obs_error, obs_index, obs_count):
    dma = pltpu.SemaphoreType.DMA
    n = len(CHUNKS)
    square = pltpu.VMEM((K * K, 128), F32)
    hbm = [pltpu.with_memory_space_constraint(v, pltpu.MemorySpace.HBM) for v in (ensemble, obs_value, obs_error, obs_index, obs_count.reshape(1, BROWS))]
    return pl.pallas_call(
        kernel,
        out_shape=jax.ShapeDtypeStruct(ensemble.shape, F32),
        in_specs=[pl.BlockSpec(memory_space=pltpu.MemorySpace.HBM)] * 5,
        out_specs=pl.BlockSpec(memory_space=pl.ANY),
        scratch_shapes=[
            pltpu.SMEM((1, BROWS), jnp.int32),
            pltpu.VMEM((BROWS, 1, OBS), F32), pltpu.VMEM((BROWS, 1, OBS), F32), pltpu.VMEM((BROWS, 1, OBS), jnp.int32), dma((5,)),
            pltpu.VMEM((K, ROWS, COLS, VALS), F32),
            pltpu.VMEM((COLS, 4 * ROWS, OBS), F32),
            pltpu.VMEM((NR, 4 * ROWS, OBS), F32),
            pltpu.VMEM((ROWS + 2, COLS + 2, K, OBS), F32),
            pltpu.VMEM((ROWS + 2, 2, COLS + 2 * GROUP, OBS), F32),
            pltpu.VMEM((ROWS, COLS, VALS), F32),
            pltpu.VMEM((2 * PAIRS, DEEP * 128), F32),
            pltpu.VMEM((256, DEEP * 128), F32),
            pltpu.VMEM((2 * PAIRS, DEEP * 128), F32),
            pltpu.VMEM((256, DEEP * 128), F32),
            pltpu.VMEM((MINE, ROWS, BCOLS, VALS), F32),
            pltpu.VMEM((ROWS, BCOLS, OBS), F32),
            pltpu.VMEM((2, NM, MINE, ROWS, GROUP, OBS), F32),
            pltpu.VMEM((2, K, ROWS, GROUP, OBS), F32),
            pltpu.VMEM((PAIRS, 128), F32),
            square, square, square, square, square, square,
            pltpu.VMEM((K, ROWS, COLS, VALS), F32),
            dma((1,)), dma((1,)), dma((n,)), dma((n,)), dma((n,)),
            dma((6,)), dma((6,)), dma((n,)), dma((n,)), dma((n,)),
            dma((1,)), dma((1,)), dma((2,)), dma((2,)),
        ],
        compiler_params=pltpu.CompilerParams(collective_id=0, has_side_effects=True, vmem_limit_bytes=40 << 20),
    )(*hbm)


def solution(mesh):
    return jax.shard_map(
        local,
        mesh=mesh,
        in_specs=(
            P("member", "region", None, None),
            P(None, ("member", "region"), None),
            P(None, ("member", "region"), None),
            P(None, ("member", "region"), None),
            P(None, ("member", "region")),
        ),
        out_specs=P("member", "region", None, None),
        check_vma=False,
    )
```

```python
import functools
import math

import jax
import jax.numpy as jnp
from jax import lax
from jax.experimental import pallas as pl
from jax.experimental.pallas import tpu as pltpu
from jax.sharding import PartitionSpec as P

MESH = pl.DeviceIdType.MESH
F32 = jnp.float32
BF16 = jnp.bfloat16

SIDE = 16
OBS = 128
NS_ITERS = 6
VALS = 512
K = 24
BROWS = 32
BCOLS = 128
LOC_SCALE = 12.0
INFLATION_FACTOR = 1.1
NM = 8
NR = 16
MINE = K // NM
ROWS = BROWS // NR
COLS = BCOLS // NM
GROUP = 8
CHUNKS = [(g, i) for g in range(COLS // GROUP) for i in range(ROWS)]
AT = GROUP - 1
TERMS = [(a, b, d) for a in range(3) for b in range(a, 3) for d in range(8 if b > a else 5)]
DRIVE = 8 * len(TERMS)
PAIRS = DRIVE + K
DEEP = 8


def dev(m, r):
    return (lax.rem(m + NM, NM), lax.rem(r + NR, NR))


def remote(src, dst, send, recv, device):
    return pltpu.make_async_remote_copy(
        src_ref=src, dst_ref=dst, send_sem=send, recv_sem=recv, device_id=device, device_id_type=MESH
    )


def tri_product(dst, a, b, post):
    for ga, height in ((0, 4), (1, 4), (2, 8)):
        groups = list(range(ga, 3))
        for first in range(8 * ga, 8 * ga + 8, height):
            acc = [[None] * len(groups) for _ in range(height)]
            for k in range(K):
                bv = [b[pl.ds(k * K + 8 * gj, 8), :] for gj in groups]
                for u in range(height):
                    av = jnp.broadcast_to(a[pl.ds((first + u) * K + k, 1), :], (8, 128))
                    for n in range(len(groups)):
                        term = av * bv[n]
                        acc[u][n] = term if acc[u][n] is None else acc[u][n] + term
            for u in range(height):
                for n, gj in enumerate(groups):
                    dst[pl.ds((first + u) * K + 8 * gj, 8), :] = post(acc[u][n], first + u, gj)
    fill_lower(dst)


def fill_lower(dst):
    for i in range(8, K):
        for gj in range(i // 8):
            dst[pl.ds(i * K + 8 * gj, 8), :] = dst[pl.ds(8 * gj * K + i, 8, stride=K), :]


def unit(i, gj):
    if i // 8 != gj:
        return jnp.zeros((8, 128), F32)
    return jnp.where(lax.broadcasted_iota(jnp.int32, (8, 128), 0) == i % 8, 1.0, 0.0).astype(F32)


def same(v, i, gj):
    return v


def newton_schulz(gram, wts, p, s, t, z, rest):
    square = jnp.zeros((8, 128), F32)
    for ga in range(3):
        for gb in range(ga, 3):
            base = 8 * TERMS.index((ga, gb, 0))
            source, start = gram, base
            if ga == gb:
                source, start = rest, 64 * ga
                for d in range(8):
                    v = gram[pl.ds(base + 8 * min(d, 8 - d), 8), :]
                    rest[pl.ds(start + 8 * d, 8), :] = pltpu.roll(v, 8 - d, 0) if d > 4 else v
            for u in range(8):
                k = 8 * ga + u
                v = source[pl.ds(start + u, 8, stride=8), :]
                v = pltpu.roll(v, u, 0) if u else v
                if ga == gb:
                    v = v + (K - 1) / INFLATION_FACTOR * unit(k, gb)
                p[pl.ds(k * K + 8 * gb, 8), :] = v
                square = square + v * v * (1.0 if ga == gb else 2.0)
    norm = jnp.sqrt(jnp.sum(square, axis=0, keepdims=True))
    inv_norm = 1.0 / norm
    for k in range(K):
        for gj in range(k // 8, 3):
            rows = pl.ds(k * K + 8 * gj, 8)
            p[rows, :] = p[rows, :] * inv_norm
    fill_lower(p)

    def square_of(v, i, gj):
        rows = pl.ds(i * K + 8 * gj, 8)
        rest[rows, :] = 1.6875 * unit(i, gj) - 0.5625 * p[rows, :] + 0.0625 * v
        return v

    def factor_of(v, i, gj):
        return v + (2.25 * unit(i, gj) - 2.4375 * p[pl.ds(i * K + 8 * gj, 8), :])

    def factor(dst):
        tri_product(s, p, p, square_of)
        fill_lower(rest)
        tri_product(dst, s, rest, factor_of)

    factor(z)
    tri_product(t, p, z, same)
    tri_product(p, t, z, same)
    factor(t)
    tri_product(s, p, t, same)
    tri_product(p, s, t, same)
    tri_product(wts, z, t, same)
    factor(t)
    tri_product(z, wts, t, same)
    scale = 1.0 / jnp.sqrt(norm)

    def apply(vector):
        acc = [jnp.zeros((8, 128), F32) for _ in range(3)]
        for k in range(K):
            row = vector[k // 8][k % 8 : k % 8 + 1, :]
            for gj in range(3):
                acc[gj] = acc[gj] + z[pl.ds(k * K + 8 * gj, 8), :] * row
        return [v * scale for v in acc]

    drive = [gram[pl.ds(DRIVE + 8 * gj, 8), :] for gj in range(3)]
    mean_w = apply(apply(drive))
    root = scale * math.sqrt(K - 1)
    for j in range(K):
        row = mean_w[j // 8][j % 8 : j % 8 + 1, :]
        for gj in range(3):
            rows = pl.ds(j * K + 8 * gj, 8)
            wts[rows, :] = z[rows, :] * root + row


def gather_group(mine, places, seen_out, m, g):
    for other in range(NM):
        cols = pl.ds(other * COLS + g * GROUP, GROUP)
        for i in range(ROWS):
            index = places[i, cols, :].astype(jnp.int32)
            lane = jnp.bitwise_and(index, 127)
            tile = jnp.right_shift(index, 7)
            for u in range(MINE):
                v = [
                    jnp.take_along_axis(mine[u, i, cols, pl.ds(128 * t, 128)], lane, axis=1, mode="promise_in_bounds")
                    for t in range(4)
                ]
                low, high = jnp.where(tile < 1, v[0], v[1]), jnp.where(tile < 3, v[2], v[3])
                seen_out[g, other, u, i] = jnp.where(tile < 2, low, high)


def stack_chunk(x, obs, stack, extra, means, i):
    cols = pl.ds(0, GROUP)
    center_chunk(x, means, 0, i)
    root_weight = obs[cols, i * 4 + 0, :]
    index = obs[cols, i * 4 + 2, :].astype(jnp.int32)
    lane = jnp.bitwise_and(index, 127)
    tile = jnp.right_shift(index, 7)

    def pick(ref):
        v = [
            jnp.take_along_axis(ref[i, cols, pl.ds(128 * t, 128)], lane, axis=1, mode="promise_in_bounds")
            for t in range(4)
        ]
        low, high = jnp.where(tile < 1, v[0], v[1]), jnp.where(tile < 3, v[2], v[3])
        return jnp.where(tile < 2, low, high)

    for k in range(K):
        stack[1 + i, pl.ds(1, GROUP), k, :] = root_weight * pick(x.at[k])
    extra[1 + i, 0, pl.ds(GROUP, GROUP), :] = root_weight * (obs[cols, i * 4 + 1, :] - pick(means))
    extra[1 + i, 1, pl.ds(GROUP, GROUP), :] = jnp.bitwise_and(index, SIDE * SIDE - 1).astype(F32)


def stack_group(seen, obs, stack, extra, g):
    cols = pl.ds(g * GROUP, GROUP)
    here = pl.ds(1 + g * GROUP, GROUP)
    for i in range(ROWS):
        total = seen[g, 0, i]
        for k in range(1, K):
            total = total + seen[g, k, i]
        mean = total * (1.0 / K)
        root_weight = obs[cols, i * 4 + 0, :]
        for k in range(K):
            stack[1 + i, here, k, :] = root_weight * (seen[g, k, i] - mean)
        index = obs[cols, i * 4 + 2, :].astype(jnp.int32)
        extra[1 + i, 0, pl.ds((1 + g) * GROUP, GROUP), :] = root_weight * (obs[cols, i * 4 + 1, :] - mean)
        extra[1 + i, 1, pl.ds((1 + g) * GROUP, GROUP), :] = jnp.bitwise_and(index, SIDE * SIDE - 1).astype(F32)


def center_chunk(x, means, g, i):
    cols = pl.ds(pl.multiple_of(g * GROUP, GROUP), GROUP)
    for t in range(4):
        lanes = pl.ds(128 * t, 128)
        total = x[0, i, cols, lanes]
        for k in range(1, K):
            total = total + x[k, i, cols, lanes]
        mean = total * (1.0 / K)
        means[i, cols, lanes] = mean
        for k in range(K):
            x[k, i, cols, lanes] = x[k, i, cols, lanes] - mean


def rounded(v):
    return v.astype(BF16).astype(F32)


def gram_blocks(stack, extra, buffers, gram, blocks, m, r):
    sub = lax.broadcasted_iota(jnp.int32, (8, 128), 0)
    point_row = jnp.right_shift(sub, 2)
    center_row = (jnp.bitwise_and(jnp.right_shift(sub, 1), 1) * 8).astype(F32) + 3.5
    center_col = (jnp.bitwise_and(sub, 1) * 8).astype(F32) + 3.5
    zero = jnp.zeros((8, 128), F32)
    for n, (tr, c) in enumerate(blocks):
        lhs, loc = buffers[n // DEEP % 2]
        lanes = pl.ds(n % DEEP * 128, 128)
        cell = jnp.broadcast_to(extra[tr, 1, pl.ds(AT + c, 1), :], (8, 128)).astype(jnp.int32)
        cell_row = jnp.right_shift(cell, 4).astype(F32)
        cell_col = jnp.bitwise_and(cell, 15).astype(F32)
        row = r * ROWS + tr - 1
        column = m * COLS + c - 1
        inside = jnp.logical_and(jnp.logical_and(column >= 0, column < BCOLS), jnp.logical_and(row >= 0, row < BROWS))
        di = tr - 1 - point_row
        dy = (SIDE * di).astype(F32) + cell_row - center_row
        keep = jnp.logical_and(jnp.abs(di) <= 1, inside)
        reach = {}
        for e in (-1, 0, 1):
            if 0 <= c - 1 + e < COLS:
                dx = cell_col - center_col - float(SIDE * e)
                weight = jnp.exp((dy * dy + dx * dx) * (-1.0 / (2.0 * LOC_SCALE * LOC_SCALE)))
                reach[c - 1 + e] = jnp.where(keep, weight, 0.0)
        for col in range(COLS):
            high = low = zero
            if col in reach:
                high = rounded(reach[col])
                low = reach[col] - high
            loc[pl.ds(8 * col, 8), lanes] = high
            loc[pl.ds(128 + 8 * col, 8), lanes] = low
        members = [stack[tr, c, pl.ds(8 * gj, 8), :] for gj in range(3)]
        turned = [[pltpu.roll(v, 8 - d, 0) if d else v for d in range(8)] for v in members]
        innovation = jnp.broadcast_to(extra[tr, 0, pl.ds(AT + c, 1), :], (8, 128))
        pieces = [members[ga] * turned[gb][d] for ga, gb, d in TERMS] + [innovation * v for v in members]
        for t in range(PAIRS // 16):
            both = jnp.concatenate(pieces[2 * t : 2 * t + 2], axis=0)
            lhs[pl.ds(16 * t, 16), lanes] = both
            lhs[pl.ds(PAIRS + 16 * t, 16), lanes] = both - rounded(both)
        if n % DEEP == DEEP - 1 or n == len(blocks) - 1:
            depth = pl.ds(0, 128 * (n % DEEP + 1))
            dims = (((1,), (1,)), ((), ()))
            high = lax.dot_general(lhs[pl.ds(0, PAIRS), depth], loc[:, depth], dims, precision=lax.Precision.DEFAULT, preferred_element_type=F32)
            low = lax.dot_general(
                lhs[pl.ds(PAIRS, PAIRS), depth], loc[pl.ds(0, 128), depth], dims, precision=lax.Precision.DEFAULT, preferred_element_type=F32
            )
            gram[...] = gram[...] + ((low + high[:, 128:]) + high[:, :128])


def update_members(x, means, wts, result, g, i, others):
    cols = pl.ds(pl.multiple_of(g * GROUP, GROUP), GROUP)
    sub = lax.broadcasted_iota(jnp.int32, (8, 128), 0)
    lane = lax.broadcasted_iota(jnp.int32, (8, 128), 1)
    base = (g * GROUP + sub) * 8 + i * 4 + jnp.bitwise_and(jnp.right_shift(lane, 3), 1)
    members = [other * MINE + u for other in others for u in range(MINE)]
    for h in range(2):
        index = base + 2 * h
        acc = [[means[i, cols, pl.ds(128 * (2 * f + h), 128)] for f in range(2)] for _ in members]
        for j in range(K):
            xs = [x[j, i, cols, pl.ds(128 * (2 * f + h), 128)] for f in range(2)]
            for u, k in enumerate(members):
                row = jnp.broadcast_to(wts[pl.ds(j * K + k, 1), :], (8, 128))
                wv = jnp.take_along_axis(row, index, axis=1, mode="promise_in_bounds")
                for f in range(2):
                    acc[u][f] = acc[u][f] + wv * xs[f]
        for u, k in enumerate(members):
            for f in range(2):
                result[k, i, cols, pl.ds(128 * (2 * f + h), 128)] = acc[u][f]


def kernel(
    ens, value_in, error_in, index_in, count_in, out,
    count,    value, error, index, load,
    x, obs, packed, stack, extra, means, lhs0, loc0, lhs1, loc1, mine, places, seen_out, seen, gram, wts, y, z, mm, tmp, rest, result,
    obs_send, obs_recv, in_send, in_recv, own_in, halo_send, halo_recv, out_send, out_recv, own_out, place_send, place_recv, seen_send, seen_recv,
):
    m = lax.axis_index("member")
    r = lax.axis_index("region")

    loads = [
        pltpu.make_async_copy(src, dst, load.at[n])
        for n, (src, dst) in enumerate(((value_in, value), (error_in, error), (index_in, index), (count_in, count), (ens, mine)))
    ]
    barrier = pltpu.get_barrier_semaphore()
    around = [dev(m + d, r) for d in range(1, NM)] + [dev(m, r + d) for d in range(1, NR)]
    around += [dev(m + a, r + b) for a in (-1, 1) for b in (-1, 1)]
    for device in around:
        pl.semaphore_signal(barrier, inc=1, device_id=device, device_id_type=MESH)
    for copy in loads:
        copy.start()
    for copy in loads[:4]:
        copy.wait()
    sub = lax.broadcasted_iota(jnp.int32, (8, OBS), 0)
    slot = lax.broadcasted_iota(jnp.int32, (8, OBS), 1)
    for n in range(BROWS // 8):
        rows = pl.ds(8 * n, 8)
        limit = jnp.zeros((8, OBS), jnp.int32)
        for u in range(8):
            limit = jnp.where(sub == u, count[0, 8 * n + u], limit)
        live = jnp.where(slot < limit, 1.0, 0.0).astype(F32)
        fields = (jnp.sqrt(live / error[rows, 0, :]), value[rows, 0, :], index[rows, 0, :].astype(F32))
        for f, field in enumerate(fields):
            for u in range(8):
                to = 8 * n + u
                packed[to // ROWS, to % ROWS * 4 + f, :] = field[u]
    pl.semaphore_wait(barrier, len(around))

    def obs_copy(d):
        other = lax.rem(r + d, NR)
        return remote(packed.at[other], obs.at[r], obs_send.at[0], obs_recv.at[0], (m, other))

    for d in range(1, NR):
        obs_copy(d).start()

    def in_copy(q, d):
        g, i = q // ROWS, q % ROWS
        other = lax.rem(m + d, NM)
        src = mine.at[:, i, pl.ds(pl.multiple_of(other * COLS + g * GROUP, GROUP), GROUP), :]
        dst = x.at[pl.ds(m * MINE, MINE), i, pl.ds(pl.multiple_of(g * GROUP, GROUP), GROUP), :]
        return remote(src, dst, in_send.at[q], in_recv.at[q], (other, r))

    def in_all(q):
        g, i = q // ROWS, q % ROWS
        part = x.at[pl.ds(0, K - MINE), i, pl.ds(pl.multiple_of(g * GROUP, GROUP), GROUP), :]
        return remote(part, part, in_send.at[q], in_recv.at[q], (m, r))

    def own_copy(q):
        g, i = q // ROWS, q % ROWS
        src = ens.at[:, i, pl.ds(pl.multiple_of(m * COLS + g * GROUP, GROUP), GROUP), :]
        dst = x.at[pl.ds(m * MINE, MINE), i, pl.ds(pl.multiple_of(g * GROUP, GROUP), GROUP), :]
        return pltpu.make_async_copy(src, dst, own_in.at[q])

    def send_in(q, part=range(NM)):
        for d in part:
            (in_copy(q, d) if d else own_copy(q)).start()

    loads[4].wait()
    send_in(0)
    obs[r] = packed[r]
    gram[...] = jnp.zeros_like(gram)
    obs_all = remote(packed.at[pl.ds(0, NR - 1)], obs.at[pl.ds(0, NR - 1)], obs_send.at[0], obs_recv.at[0], (m, r))
    obs_all.wait_recv()

    def place_copy(d):
        own = places.at[:, pl.ds(pl.multiple_of(m * COLS + GROUP, GROUP), GROUP), :]
        return remote(own, own, place_send.at[0], place_recv.at[0], (lax.rem(m + d, NM), r))

    def seen_copy(g, d):
        other = lax.rem(m + d, NM)
        dst = seen.at[g, pl.ds(m * MINE, MINE)]
        return remote(seen_out.at[g, other], dst, seen_send.at[g], seen_recv.at[g], (other, r))

    def seen_all(g):
        part = seen.at[g, pl.ds(0, K - MINE)]
        return remote(part, part, seen_send.at[g], seen_recv.at[g], (m, r))

    for i in range(ROWS):
        cols = pl.ds(pl.multiple_of(m * COLS + GROUP, GROUP), GROUP)
        places[i, cols, :] = obs[pl.ds(GROUP, GROUP), i * 4 + 2, :]
    for d in range(1, NM):
        place_copy(d).start()
    send_in(1)

    def halo_pair(src, dst, sem, device):
        return [remote(ref.at[a], ref.at[b], halo_send.at[sem], halo_recv.at[sem], device) for ref, a, b in zip((stack, extra), src, dst)]

    def row_halo(g, i):
        to = 3 if i == 0 else 0
        where, wide = pl.ds(1 + g * GROUP, GROUP), pl.ds((1 + g) * GROUP, GROUP)
        device = dev(m, r + (-1 if i == 0 else 1))
        return halo_pair(((1 + i, where), (1 + i, slice(None), wide)), ((to, where), (to, slice(None), wide)), ROWS * g + i, device)

    def side_halo(g):
        col, to, a = (1, COLS + 1, -1) if g == 0 else (COLS, 0, 1)
        wide, there = pl.ds((1 + g) * GROUP, GROUP), pl.ds((COLS + GROUP) * (1 - g), GROUP)
        copies = []
        for rows, to_rows, b in ((pl.ds(1, 2), pl.ds(1, 2), 0), (1, 3, -1), (2, 0, 1)):
            copies += halo_pair(
                ((rows, col), (rows, slice(None), wide)), ((to_rows, to), (to_rows, slice(None), there)), 4 + g, dev(m + a, r + b)
            )
        return copies

    def row_all(g, i):
        n = GROUP * K + 2 * GROUP
        return wait_for(n, ROWS * g + i)

    def side_all(g):
        return wait_for(4 * (K + 2 * GROUP), 4 + g)

    def wait_for(rows, sem):
        part = wts.at[pl.ds(0, rows), :]
        return remote(part, part, halo_send.at[sem], halo_recv.at[sem], (m, r))

    def arrive(i):
        own_copy(i).wait()
        in_all(i).wait_recv()
        stack_chunk(x, obs, stack, extra, means, i)

    arrive(0)
    for copy in row_halo(0, 0):
        copy.start()
    rest_of = places.at[:, pl.ds(0, (NM - 1) * GROUP), :]
    place_all = remote(rest_of, rest_of, place_send.at[0], place_recv.at[0], (m, r))
    place_all.wait_recv()
    gather_group(mine, places, seen_out, m, 1)
    for d in range(1, NM):
        seen_copy(1, d).start()
    seen[1, pl.ds(m * MINE, MINE)] = seen_out[1, m]

    def add(blocks):
        gram_blocks(stack, extra, ((lhs0, loc0), (lhs1, loc1)), gram, blocks, m, r)

    def own(g):
        return [(1 + i, 1 + g * GROUP + c) for i in range(ROWS) for c in range(GROUP)]

    def beyond(g):
        return [(3 * i, 1 + g * GROUP + c) for i in range(ROWS) for c in range(GROUP)]

    arrive(1)
    for copy in side_halo(0) + row_halo(0, 1):
        copy.start()
    send_in(2, (2, 6, 1, 7))
    add(own(0))
    seen_all(1).wait_recv()
    stack_group(seen, obs, stack, extra, 1)
    for copy in side_halo(1) + row_halo(1, 0) + row_halo(1, 1):
        copy.start()
    send_in(2, (3, 5, 4, 0))
    send_in(3)
    add(own(1))
    for i in range(ROWS):
        row_all(0, i).wait_recv()
    add(beyond(0))
    side_all(0).wait_recv()
    add([(tr, COLS + 1) for tr in range(4)])
    for i in range(ROWS):
        row_all(1, i).wait_recv()
    side_all(1).wait_recv()
    add(beyond(1) + [(tr, 0) for tr in range(4)])
    newton_schulz(gram, wts, y, z, mm, tmp, rest)

    def out_copy(q, d):
        g, i = q // ROWS, q % ROWS
        other = lax.rem(m + d, NM)
        src = result.at[pl.ds(other * MINE, MINE), i, pl.ds(pl.multiple_of(g * GROUP, GROUP), GROUP), :]
        dst = out.at[:, i, pl.ds(pl.multiple_of(m * COLS + g * GROUP, GROUP), GROUP), :]
        return remote(src, dst, out_send.at[q], out_recv.at[q], (other, r))

    def out_all(q):
        g, i = q // ROWS, q % ROWS
        part = result.at[pl.ds(0, K - MINE), i, pl.ds(pl.multiple_of(g * GROUP, GROUP), GROUP), :]
        return remote(part, part, out_send.at[q], out_recv.at[q], (m, r))

    def keep_copy(q):
        g, i = q // ROWS, q % ROWS
        src = result.at[pl.ds(m * MINE, MINE), i, pl.ds(pl.multiple_of(g * GROUP, GROUP), GROUP), :]
        dst = out.at[:, i, pl.ds(pl.multiple_of(m * COLS + g * GROUP, GROUP), GROUP), :]
        return pltpu.make_async_copy(src, dst, own_out.at[q])

    def chunk_out(q, carry):
        @pl.when(q >= ROWS)
        def _():
            own_copy(q).wait()
            in_all(q).wait_recv()
            center_chunk(x, means, q // ROWS, q % ROWS)

        for pair in ((2,), (6,), (3, 5), (4, 1), (7, 0)):
            update_members(x, means, wts, result, q // ROWS, q % ROWS, [lax.rem(m + d, NM) for d in pair])
            for d in pair:
                (out_copy(q, d) if d else keep_copy(q)).start()
        return carry

    lax.fori_loop(0, len(CHUNKS), chunk_out, 0)

    obs_all.wait_send()
    place_all.wait_send()
    seen_all(1).wait_send()
    for g in range(2):
        side_all(g).wait_send()
        for i in range(ROWS):
            row_all(g, i).wait_send()
    for q in range(len(CHUNKS)):
        in_all(q).wait_send()
    for q in range(len(CHUNKS)):
        keep_copy(q).wait()
        out_all(q).wait_send()
        out_all(q).wait_recv()


def local(ensemble, obs_value, obs_error, obs_index, obs_count):
    dma = pltpu.SemaphoreType.DMA
    n = len(CHUNKS)
    square = pltpu.VMEM((K * K, 128), F32)
    hbm = [pltpu.with_memory_space_constraint(v, pltpu.MemorySpace.HBM) for v in (ensemble, obs_value, obs_error, obs_index, obs_count.reshape(1, BROWS))]
    return pl.pallas_call(
        kernel,
        out_shape=jax.ShapeDtypeStruct(ensemble.shape, F32),
        in_specs=[pl.BlockSpec(memory_space=pltpu.MemorySpace.HBM)] * 5,
        out_specs=pl.BlockSpec(memory_space=pl.ANY),
        scratch_shapes=[
            pltpu.SMEM((1, BROWS), jnp.int32),
            pltpu.VMEM((BROWS, 1, OBS), F32), pltpu.VMEM((BROWS, 1, OBS), F32), pltpu.VMEM((BROWS, 1, OBS), jnp.int32), dma((5,)),
            pltpu.VMEM((K, ROWS, COLS, VALS), F32),
            pltpu.VMEM((COLS, 4 * ROWS, OBS), F32),
            pltpu.VMEM((NR, 4 * ROWS, OBS), F32),
            pltpu.VMEM((ROWS + 2, COLS + 2, K, OBS), F32),
            pltpu.VMEM((ROWS + 2, 2, COLS + 2 * GROUP, OBS), F32),
            pltpu.VMEM((ROWS, COLS, VALS), F32),
            pltpu.VMEM((2 * PAIRS, DEEP * 128), F32),
            pltpu.VMEM((256, DEEP * 128), F32),
            pltpu.VMEM((2 * PAIRS, DEEP * 128), F32),
            pltpu.VMEM((256, DEEP * 128), F32),
            pltpu.VMEM((MINE, ROWS, BCOLS, VALS), F32),
            pltpu.VMEM((ROWS, BCOLS, OBS), F32),
            pltpu.VMEM((2, NM, MINE, ROWS, GROUP, OBS), F32),
            pltpu.VMEM((2, K, ROWS, GROUP, OBS), F32),
            pltpu.VMEM((PAIRS, 128), F32),
            square, square, square, square, square, square,
            pltpu.VMEM((K, ROWS, COLS, VALS), F32),
            dma((1,)), dma((1,)), dma((n,)), dma((n,)), dma((n,)),
            dma((6,)), dma((6,)), dma((n,)), dma((n,)), dma((n,)),
            dma((1,)), dma((1,)), dma((2,)), dma((2,)),
        ],
        compiler_params=pltpu.CompilerParams(collective_id=0, has_side_effects=True, vmem_limit_bytes=40 << 20),
    )(*hbm)


def solution(mesh):
    return jax.shard_map(
        local,
        mesh=mesh,
        in_specs=(
            P("member", "region", None, None),
            P(None, ("member", "region"), None),
            P(None, ("member", "region"), None),
            P(None, ("member", "region"), None),
            P(None, ("member", "region")),
        ),
        out_specs=P("member", "region", None, None),
        check_vma=False,
    )
```
